32 devices in a mesh: lon: 8 (over y, x, core), lat: 4 (over z).
Axes of the slice: x: 2, y: 2, z: 4, core: 2. Of those that a mesh axis runs over, the one named last changes fastest.
Arguments:
- fields: bfloat16 [4, 128, 32, 1024], P(None, None, 'lat', 'lon'), may hold values from -12 to 12
- bracket: int32 [32, 32, 1024], P(None, 'lat', 'lon'), may hold values from 0 to 126, as said below
- fraction: bfloat16 [32, 32, 1024], P(None, 'lat', 'lon'), may hold values from 0 to 1
Outputs:
- on_pressure: bfloat16 [4, 32, 32, 1024], P(None, None, ('lat', 'lon'))
- zonal_mean: float32 [4, 32, 32], P(None, None, ('lat', 'lon'))
- meridional: float32 [4, 32, 32], P(None, None, ('lat', 'lon'))
The draws below stay inside these ranges and needn't reach their ends.
Inputs may be any that keep to these rules, and one draw needn't show every extreme that they name: bracket[p, r, c] - min(p * 4, 112) lies in 0 to 14 for every column, and each of these offsets occurs.
All inputs are finite; a program needn't handle non-finite values.
Results may differ from the reference program's by a relative error of at most 0.0012.
Values may be sent and summed in bfloat16 or wider, within the bound.
A program may use at most 128 MiB of HBM per device.

```python
import jax
import jax.numpy as jnp
from jax import lax

VARS = 4
LEV = 128
PLEV = 32
WINDOW = 16
NLAT = 32
NLON = 1024


def draw_fields(key, part):
    key_noise = jax.random.fold_in(key, 11)
    key_offset = jax.random.fold_in(key, 12)
    noise_part = jnp.clip(jax.random.normal(key_noise, (VARS, LEV, NLAT, NLON), jnp.float32), -4.0, 4.0)
    offset = jax.random.uniform(key_offset, (VARS, LEV, NLAT, 1), jnp.float32, -4.0, 4.0)
    values = noise_part + offset
    return values.astype(jnp.bfloat16)


def draw_bracket(key, part):
    key_offset = jax.random.fold_in(key, 21)
    level_step = LEV // PLEV
    pressure_index = jnp.arange(PLEV, dtype=jnp.int32).reshape(PLEV, 1, 1)
    window_base = jnp.minimum(pressure_index * level_step, LEV - WINDOW)
    offsets = jax.random.randint(key_offset, (PLEV, NLAT, NLON), 0, WINDOW - 1, dtype=jnp.int32)
    return (window_base + offsets).astype(jnp.int32)


def shard_levels(key, shape, cuts, low, largest):
    def one(dim, blocks):
        steps = jax.random.uniform(jax.random.fold_in(jax.random.fold_in(key, 6), dim), (blocks,), jnp.float32, low / len(cuts), largest / len(cuts))
        return jnp.repeat(jnp.exp(steps), shape[dim] // blocks).reshape((-1,) + (1,) * (len(shape) - dim - 1))

    level = one(*cuts[0])
    for cut in cuts[1:]:
        level = level * one(*cut)
    return level


def setup_inputs(seed: int = 0) -> dict:
    streams_of = jax.random.split(jax.random.key(seed), 4)
    return {
        "fields": draw_fields(jax.random.fold_in(streams_of[3], 71), 0),
        "bracket": draw_bracket(jax.random.fold_in(streams_of[3], 71), 0),
        "fraction": jnp.clip(1.0 * jax.random.uniform(streams_of[2], (PLEV, NLAT, NLON), jnp.float32) ** shard_levels(streams_of[2], (PLEV, NLAT, NLON), ((1, 4), (2, 8)), -0.2, 0.2), 0.0, 1.0).astype(jnp.bfloat16),
    }


def interpolate(block, bracket, fraction):
    index = jnp.broadcast_to(bracket[None], (block.shape[0],) + bracket.shape)
    lower_level = jnp.take_along_axis(block, index, axis=1).astype(jnp.float32)
    upper_level = jnp.take_along_axis(block, index + 1, axis=1).astype(jnp.float32)
    weight = fraction.astype(jnp.float32)[None]
    return (lower_level + weight * (upper_level - lower_level)).astype(jnp.bfloat16)


def reference(fields, bracket, fraction):
    on_pressure = lax.map(lambda single: interpolate(single[None], bracket, fraction)[0], fields)
    zonal_mean = jnp.sum(on_pressure.astype(jnp.float32), axis=3) / jnp.float32(NLON)
    centered = 0.5 * (zonal_mean[:, :, 2:] - zonal_mean[:, :, :-2])
    first_row = zonal_mean[:, :, 1:2] - zonal_mean[:, :, 0:1]
    last_row = zonal_mean[:, :, -1:] - zonal_mean[:, :, -2:-1]
    meridional = jnp.concatenate([first_row, centered, last_row], axis=2)
    return on_pressure, zonal_mean, meridional
```

```python
import functools

import jax
import jax.numpy as jnp
from jax import lax
from jax.experimental import pallas as pl
from jax.experimental.pallas import tpu as pltpu
from jax.sharding import PartitionSpec as P

WINDOW = 16
TILE = 8
PACK = 16
MESH = pl.DeviceIdType.MESH
HUB = 2


def select_pair(levels, masks):
    bit = len(levels) // 2
    for mask in masks:
        levels = [
            jnp.where(mask, levels[k + bit], levels[k]) if k + bit < len(levels) else levels[k]
            for k in range(bit + 1)
        ]
        bit //= 2
    return levels


def partner(me, k, count):
    if count & (count - 1):
        return (me + k) % count, (me + count - k) % count
    peer, bit = me, 1
    while bit < count:
        if k & bit:
            peer = peer + bit - 2 * bit * ((me // bit) % 2)
        bit *= 2
    return peer, peer


def interpolate(pair, fields, bracket, fraction, send):
    _, level_count, both_rows, lons = fields.shape
    plev_count, row_count, _ = bracket.shape
    level_step = level_count // plev_count
    group_size = min(TILE, plev_count)

    def block(tile):
        where = [tile * PACK + half for half in range(0, PACK, TILE)]
        rows = [pl.ds(pl.multiple_of(at % row_count, TILE), TILE) for at in where]
        packed = pl.ds(pl.multiple_of(tile * PACK, PACK), PACK)
        loaded, groups = {}, [[], []]
        for p in range(plev_count):
            base = min(p * level_step, level_count - WINDOW)
            for k in range(base, base + WINDOW):
                if k not in loaded:
                    loaded[k] = fields[pair, k, packed, :]
            offset = (jnp.concatenate([bracket[p, r, :] for r in rows]) - base).astype(jnp.int16)
            masks, bit = [], WINDOW // 2
            while bit:
                masks.append((offset & jnp.int16(bit)) != jnp.int16(0))
                bit //= 2
            lower, upper = select_pair([loaded[base + k] for k in range(WINDOW)], masks)
            lower, upper = lower.astype(jnp.float32), upper.astype(jnp.float32)
            weight = jnp.concatenate([fraction[p, r, :] for r in rows]).astype(jnp.float32)
            value = lower + weight * (upper - lower)
            groups[0].append(value[:TILE])
            groups[1].append(value[TILE:])
            if len(groups[0]) == group_size:
                for half in range(2):
                    by_row = jnp.transpose(jnp.stack(groups[half]), (1, 0, 2)).astype(jnp.bfloat16)
                    v = 2 * pair + where[half] // row_count
                    send[v, rows[half], p + 1 - group_size : p + 1, :] = by_row
                groups = [[], []]

    if both_rows == PACK:
        block(0)
    else:
        pl.loop(0, both_rows // PACK)(block)


def exchange(
    lon_count, lat_count, count, fields_hbm, bracket_hbm, fraction_hbm,
    out_ref, zonal, merid,
    fields, bracket, fraction, send, sums, got, cross,
    in_sem, field_sem, send_sem, recv_sem, sum_send, sum_recv, edge_send, edge_recv,
):
    var_count, row_count, plev_count, lons = send.shape
    pair_count = var_count // 2
    own = row_count // lon_count
    width = var_count * plev_count
    me = lax.axis_index("lon")
    band = lax.axis_index("lat")
    next_band = (band + 1) % lat_count
    prev_band = (band + lat_count - 1) % lat_count
    first = me == 0
    last = me == lon_count - 1
    up = band < lat_count - 1
    down = band > 0
    my_lons = pl.ds(pl.multiple_of(me * lons, 128), lons)
    peers = [partner(me, k, lon_count)[0] for k in range(lon_count - 1, 0, -1)]

    barrier = pltpu.get_barrier_semaphore()
    for peer in peers:
        pl.semaphore_signal(barrier, inc=1, device_id={"lon": peer}, device_id_type=MESH)

    @pl.when(jnp.logical_and(first, down))
    def _():
        for l in range(lon_count):
            pl.semaphore_signal(barrier, inc=1, device_id={"lon": l, "lat": prev_band}, device_id_type=MESH)

    @pl.when(jnp.logical_and(last, up))
    def _():
        for l in range(lon_count):
            pl.semaphore_signal(barrier, inc=1, device_id={"lon": l, "lat": next_band}, device_id_type=MESH)

    get_bracket = pltpu.make_async_copy(bracket_hbm, bracket, in_sem.at[0])
    get_fraction = pltpu.make_async_copy(fraction_hbm, fraction, in_sem.at[1])
    get_bracket.start()
    get_fraction.start()
    for v in range(var_count):
        pltpu.make_async_copy(
            fields_hbm.at[v],
            fields.at[v // 2, :, pl.ds(v % 2 * row_count, row_count)],
            field_sem.at[v // 2],
        ).start()

    def send_block(peer, pair):
        some = pl.ds(2 * pair, 2)
        pltpu.make_async_remote_copy(
            src_ref=send.at[some, pl.ds(peer * own, own)],
            dst_ref=out_ref.at[some, :, :, my_lons],
            send_sem=send_sem.at[0],
            recv_sem=recv_sem.at[0],
            device_id={"lon": peer},
            device_id_type=MESH,
        ).start()

    def send_sums(peer):
        pltpu.make_async_remote_copy(
            src_ref=sums.at[pl.ds(peer * own, own + 2)],
            dst_ref=got.at[me],
            send_sem=sum_send.at[0],
            recv_sem=sum_recv.at[0],
            device_id={"lon": peer},
            device_id_type=MESH,
        ).start()

    def send_edge(row, lon, lat):
        pltpu.make_async_remote_copy(
            src_ref=sums.at[row],
            dst_ref=cross.at[me],
            send_sem=edge_send.at[0],
            recv_sem=edge_recv.at[0],
            device_id={"lon": lon, "lat": lat},
            device_id_type=MESH,
        ).start()

    def to_hubs(go, *args):
        for h in range(HUB):
            pl.when(me != h)(functools.partial(go, h, *args))

    def to_others(go, *args):
        for peer in peers:
            pl.when(peer >= HUB)(functools.partial(go, peer, *args))

    sums[0] = jnp.zeros((1, width), jnp.float32)
    sums[row_count + 1] = jnp.zeros((1, width), jnp.float32)
    get_bracket.wait()
    get_fraction.wait()
    for pair in range(pair_count):
        pltpu.make_async_copy(fields.at[pair], fields.at[pair], field_sem.at[pair]).wait()
        interpolate(pair, fields, bracket, fraction, send)
        if pair == 0:
            beyond = up.astype(jnp.int32) + down.astype(jnp.int32)
            pl.semaphore_wait(barrier, lon_count - 1 + beyond)
        if pair < pair_count - 1:
            to_hubs(send_block, pair)

    ones = jnp.ones((TILE, lons), jnp.bfloat16)

    def add_up(at):
        two = jnp.concatenate([send[:, at + r].reshape(width, lons) for r in range(2)])
        total = lax.dot_general(
            ones, two, (((1,), (1,)), ((), ())), preferred_element_type=jnp.float32
        )
        sums[at + 1] = total[0:1, :width]
        sums[at + 2] = total[0:1, width:]

    if row_count == TILE:
        for at in range(0, row_count, 2):
            add_up(at)
    else:
        pl.loop(0, row_count // 2)(lambda half: add_up(2 * half))

    to_hubs(send_sums)
    to_others(send_sums)
    pl.when(up)(lambda: send_edge(row_count, 0, next_band))
    pl.when(down)(lambda: send_edge(1, lon_count - 1, prev_band))
    to_hubs(send_block, pair_count - 1)
    for pair in range(pair_count):
        to_others(send_block, pair)

    out_ref[:, :, :, my_lons] = send[:, pl.ds(me * own, own)]
    got[me] = sums[pl.ds(me * own, own + 2)]
    all_sums = got.at[pl.ds(0, lon_count - 1)]
    pltpu.make_async_copy(all_sums, all_sums, sum_recv.at[0]).wait()

    def mean_of(parts):
        total = parts[0]
        for part in parts[1:]:
            total = total + part
        return total / count

    here = [mean_of([got[l, j] for l in range(lon_count)]) for j in range(own + 2)]
    for j in range(own):
        for v in range(var_count):
            zonal[v, j : j + 1, :] = here[j + 1][:, v * plev_count : (v + 1) * plev_count]

    @pl.when(jnp.logical_or(jnp.logical_and(first, down), jnp.logical_and(last, up)))
    def _():
        pltpu.make_async_copy(cross, cross, edge_recv.at[0]).wait()

    beyond_edge = mean_of([cross[l] for l in range(lon_count)])
    bottom = jnp.logical_and(first, band == 0)
    top = jnp.logical_and(last, band == lat_count - 1)
    for j in range(own):
        below, middle, above = here[j : j + 3]
        scale = jnp.float32(0.5)
        if j == 0:
            below = jnp.where(bottom, middle, jnp.where(first, beyond_edge, below))
            scale = jnp.where(bottom, 1.0, scale)
        if j == own - 1:
            above = jnp.where(top, middle, jnp.where(last, beyond_edge, above))
            scale = jnp.where(top, 1.0, scale)
        slope = scale * (above - below)
        for v in range(var_count):
            merid[v, j : j + 1, :] = slope[:, v * plev_count : (v + 1) * plev_count]

    pltpu.make_async_copy(all_sums, all_sums, sum_send.at[0]).wait()

    @pl.when(jnp.logical_and(up, down))
    def _():
        two = sums.at[pl.ds(0, 2)]
        pltpu.make_async_copy(two, two, edge_send.at[0]).wait()

    @pl.when(up != down)
    def _():
        one = sums.at[pl.ds(0, 1)]
        pltpu.make_async_copy(one, one, edge_send.at[0]).wait()

    landed = out_ref.at[:, :, :, pl.ds(0, (lon_count - 1) * lons)]
    pltpu.make_async_copy(landed, landed, recv_sem.at[0]).wait()
    left = send.at[:, pl.ds(0, row_count - own)]
    pltpu.make_async_copy(left, left, send_sem.at[0]).wait()


def finish(rows_vmem, zonal_vmem, merid_vmem, out_hbm, zonal_hbm, merid_hbm, sem):
    puts = [
        pltpu.make_async_copy(rows_vmem, out_hbm, sem.at[0]),
        pltpu.make_async_copy(zonal_vmem, zonal_hbm, sem.at[1]),
        pltpu.make_async_copy(merid_vmem, merid_hbm, sem.at[2]),
    ]
    for put in puts:
        put.start()
    for put in puts:
        put.wait()


def shards(lon_count, lat_count, fields, bracket, fraction):
    var_count, level_count, row_count, lons = fields.shape
    plev_count = bracket.shape[0]
    own = row_count // lon_count
    width = var_count * plev_count
    dma = pltpu.SemaphoreType.DMA
    anywhere = pl.BlockSpec(memory_space=pl.ANY)
    room = 2 * fields.size + 4 * bracket.size + 2 * fraction.size * (1 + var_count)
    in_vmem = pl.BlockSpec(memory_space=pltpu.VMEM)
    rows_shape = (var_count, own, plev_count, lons * lon_count)
    mean_shape = (var_count, own, plev_count)
    inputs = [pltpu.with_memory_space_constraint(x, pltpu.HBM) for x in (fields, bracket, fraction)]
    held = pl.pallas_call(
        functools.partial(exchange, lon_count, lat_count, float(lons * lon_count)),
        out_shape=(
            pltpu.VMEM(rows_shape, jnp.bfloat16),
            pltpu.VMEM(mean_shape, jnp.float32),
            pltpu.VMEM(mean_shape, jnp.float32),
        ),
        in_specs=[anywhere] * 3,
        out_specs=(in_vmem,) * 3,
        scratch_shapes=[
            pltpu.VMEM((var_count // 2, level_count, 2 * row_count, lons), fields.dtype),
            pltpu.VMEM(bracket.shape, bracket.dtype),
            pltpu.VMEM(fraction.shape, fraction.dtype),
            pltpu.VMEM((var_count, row_count, plev_count, lons), jnp.bfloat16),
            pltpu.VMEM((row_count + 2, 1, width), jnp.float32),
            pltpu.VMEM((lon_count, own + 2, 1, width), jnp.float32),
            pltpu.VMEM((lon_count, 1, width), jnp.float32),
            dma((2,)),
            dma((var_count // 2,)),
            dma((1,)),
            dma((1,)),
            dma((1,)),
            dma((1,)),
            dma((1,)),
            dma((1,)),
        ],
        compiler_params=pltpu.CompilerParams(
            collective_id=0, has_side_effects=True, vmem_limit_bytes=room + (8 << 20)
        ),
    )(*inputs)
    held = [pltpu.with_memory_space_constraint(x, pltpu.VMEM) for x in held]
    on_pressure, zonal_mean, meridional = pl.pallas_call(
        finish,
        out_shape=(
            jax.ShapeDtypeStruct(rows_shape, jnp.bfloat16),
            jax.ShapeDtypeStruct(mean_shape, jnp.float32),
            jax.ShapeDtypeStruct(mean_shape, jnp.float32),
        ),
        in_specs=[in_vmem] * 3,
        out_specs=(anywhere,) * 3,
        scratch_shapes=[dma((3,))],
        compiler_params=pltpu.CompilerParams(vmem_limit_bytes=8 << 20),
    )(*held)
    return (
        on_pressure.transpose(0, 2, 1, 3),
        zonal_mean.transpose(0, 2, 1),
        meridional.transpose(0, 2, 1),
    )


def solution(mesh):
    return jax.shard_map(
        functools.partial(shards, mesh.shape["lon"], mesh.shape["lat"]),
        mesh=mesh,
        in_specs=(P(None, None, "lat", "lon"), P(None, "lat", "lon"), P(None, "lat", "lon")),
        out_specs=(
            P(None, None, ("lat", "lon"), None),
            P(None, None, ("lat", "lon")),
            P(None, None, ("lat", "lon")),
        ),
        check_vma=False,
    )
```

```python
import functools
import math

import jax
import jax.numpy as jnp
from jax import lax
from jax.experimental import pallas as pl
from jax.experimental.pallas import tpu as pltpu
from jax.sharding import PartitionSpec as P

WINDOW = 16
TILE = 8
PACK = 16
MESH = pl.DeviceIdType.MESH
HUB = 2
PARTS = (2, 2)


def select_pair(levels, masks):
    bit = len(levels) // 2
    for mask in masks:
        levels = [
            jnp.where(mask, levels[k + bit], levels[k]) if k + bit < len(levels) else levels[k]
            for k in range(bit + 1)
        ]
        bit //= 2
    return levels


def partner(me, k, count):
    if count & (count - 1):
        return (me + k) % count, (me + count - k) % count
    peer, bit = me, 1
    while bit < count:
        if k & bit:
            peer = peer + bit - 2 * bit * ((me // bit) % 2)
        bit *= 2
    return peer, peer


def interpolate(pair, levels, fields, bracket, fraction, send):
    _, level_count, both_rows, lons = fields.shape
    plev_count, row_count, _ = bracket.shape
    level_step = level_count // plev_count
    group_size = min(TILE, plev_count)

    def block(tile):
        where = [tile * PACK + half for half in range(0, PACK, TILE)]
        rows = [pl.ds(pl.multiple_of(at % row_count, TILE), TILE) for at in where]
        packed = pl.ds(pl.multiple_of(tile * PACK, PACK), PACK)
        loaded, groups = {}, [[], []]
        for p in levels:
            base = min(p * level_step, level_count - WINDOW)
            for k in range(base, base + WINDOW):
                if k not in loaded:
                    loaded[k] = fields[pair, k, packed, :]
            offset = (jnp.concatenate([bracket[p, r, :] for r in rows]) - base).astype(jnp.int16)
            masks, bit = [], WINDOW // 2
            while bit:
                masks.append((offset & jnp.int16(bit)) != jnp.int16(0))
                bit //= 2
            lower, upper = select_pair([loaded[base + k] for k in range(WINDOW)], masks)
            lower, upper = lower.astype(jnp.float32), upper.astype(jnp.float32)
            weight = jnp.concatenate([fraction[p, r, :] for r in rows]).astype(jnp.float32)
            value = lower + weight * (upper - lower)
            groups[0].append(value[:TILE])
            groups[1].append(value[TILE:])
            if len(groups[0]) == group_size:
                for half in range(2):
                    by_row = jnp.transpose(jnp.stack(groups[half]), (1, 0, 2)).astype(jnp.bfloat16)
                    v = 2 * pair + where[half] // row_count
                    send[v, rows[half], p + 1 - group_size : p + 1, :] = by_row
                groups = [[], []]

    if both_rows == PACK:
        block(0)
    else:
        pl.loop(0, both_rows // PACK)(block)


def exchange(
    lon_count, lat_count, count, fields_hbm, bracket_hbm, fraction_hbm,
    out_ref, zonal, merid,
    fields, bracket, fraction, send, sums, got, cross,
    in_sem, field_sem, send_sem, recv_sem, sum_send, sum_recv, edge_send, edge_recv, go,
):
    var_count, row_count, plev_count, lons = send.shape
    pair_count = var_count // 2
    own = row_count // lon_count
    width = var_count * plev_count
    me = lax.axis_index("lon")
    band = lax.axis_index("lat")
    next_band = (band + 1) % lat_count
    prev_band = (band + lat_count - 1) % lat_count
    first = me == 0
    last = me == lon_count - 1
    up = band < lat_count - 1
    down = band > 0
    my_lons = pl.ds(pl.multiple_of(me * lons, 128), lons)
    steps = range(lon_count - 1, 0, -1)
    peers = [partner(me, k, lon_count)[0] for k in steps]
    others = [(peer, (me // 2) % 2 != (k // 2) % 2) for k, peer in zip(steps, peers)]
    hub = me < HUB
    far = me >= lon_count - 2
    late = jnp.logical_and(me % 2 == 1, jnp.logical_not(jnp.logical_or(hub, far)))
    early = jnp.logical_or(far, late)
    full = jnp.logical_not(early)

    get_bracket = pltpu.make_async_copy(bracket_hbm, bracket, in_sem.at[0])
    get_fraction = pltpu.make_async_copy(fraction_hbm, fraction, in_sem.at[1])
    get_bracket.start()
    get_fraction.start()

    def get_pair(pair):
        for half in range(2):
            pltpu.make_async_copy(
                fields_hbm.at[2 * pair + half],
                fields.at[pair, :, pl.ds(half * row_count, row_count)],
                field_sem.at[pair],
            ).start()

    for pair in range(pair_count):
        get_pair(pair)

    barrier = pltpu.get_barrier_semaphore()

    def greet(peer, lat):
        pl.semaphore_signal(barrier, inc=1, device_id={"lon": peer, "lat": lat}, device_id_type=MESH)

    for peer in peers:
        listens = jnp.logical_or(jnp.logical_or(hub, peer % 2 == 0), jnp.logical_or(peer < HUB, peer >= lon_count - 2))
        pl.when(listens)(functools.partial(greet, peer, band))

    waiting = [l for l in range(lon_count - 2) if l < HUB or l % 2 == 0]

    @pl.when(jnp.logical_and(first, down))
    def _():
        for l in waiting:
            greet(l, prev_band)

    @pl.when(jnp.logical_and(last, up))
    def _():
        for l in waiting:
            greet(l, next_band)

    def send_block(peer, some, levels=slice(None)):
        pltpu.make_async_remote_copy(
            src_ref=send.at[some, pl.ds(peer * own, own), levels],
            dst_ref=out_ref.at[some, :, levels, my_lons],
            send_sem=send_sem.at[0],
            recv_sem=recv_sem.at[0],
            device_id={"lon": peer},
            device_id_type=MESH,
        ).start()

    def send_sums(peer):
        pltpu.make_async_remote_copy(
            src_ref=sums.at[pl.ds(peer * own, own + 2)],
            dst_ref=got.at[me],
            send_sem=sum_send.at[0],
            recv_sem=sum_recv.at[0],
            device_id={"lon": peer},
            device_id_type=MESH,
        ).start()

    def send_edge(row, lon, lat):
        pltpu.make_async_remote_copy(
            src_ref=sums.at[row],
            dst_ref=cross.at[me],
            send_sem=edge_send.at[0],
            recv_sem=edge_recv.at[0],
            device_id={"lon": lon, "lat": lat},
            device_id_type=MESH,
        ).start()

    def to_hubs(act, *args):
        for h in range(HUB):
            pl.when(me != h)(functools.partial(act, h, *args))

    def to_others(act, *args):
        for peer in peers:
            pl.when(peer >= HUB)(functools.partial(act, peer, *args))

    sums[0] = jnp.zeros((1, width), jnp.float32)
    sums[row_count + 1] = jnp.zeros((1, width), jnp.float32)
    get_bracket.wait()
    get_fraction.wait()
    whole = pl.ds(0, var_count)
    for pair in range(pair_count):
        pltpu.make_async_copy(fields.at[pair], fields.at[pair], field_sem.at[pair]).wait()
        some = pl.ds(2 * pair, 2)
        parts = PARTS[pair]
        for part in range(parts):
            count_here = plev_count // parts
            low = part * count_here
            interpolate(pair, range(low, low + count_here), fields, bracket, fraction, send)

            @pl.when(early)
            def _():
                if pair == 0 and part == 0:
                    pl.semaphore_wait(barrier, jnp.where(far, lon_count - 1, HUB))
                send_block(0, some, pl.ds(low, count_here))
                if pair == 0 and part == parts - 1:
                    pl.when(late)(functools.partial(send_block, 1, some))

    ones = jnp.ones((TILE, lons), jnp.bfloat16)

    def add_up(at):
        two = jnp.concatenate([send[:, at + r].reshape(width, lons) for r in range(2)])
        total = lax.dot_general(
            ones, two, (((1,), (1,)), ((), ())), preferred_element_type=jnp.float32
        )
        sums[at + 1] = total[0:1, :width]
        sums[at + 2] = total[0:1, width:]

    if row_count == TILE:
        for at in range(0, row_count, 2):
            add_up(at)
    else:
        pl.loop(0, row_count // 2)(lambda half: add_up(2 * half))

    def send_edges():
        pl.when(up)(lambda: send_edge(row_count, 0, next_band))
        pl.when(down)(lambda: send_edge(1, lon_count - 1, prev_band))

    def open_to(peer):
        pl.semaphore_signal(go, inc=1, device_id={"lon": peer}, device_id_type=MESH)

    @pl.when(full)
    def _():
        beyond = up.astype(jnp.int32) + down.astype(jnp.int32)
        pl.semaphore_wait(barrier, lon_count - 1 + beyond)
        pl.when(jnp.logical_not(hub))(lambda: open_to(me + 1))

        @pl.when(me == lon_count - 4)
        def _():
            open_to(lon_count - 2)
            open_to(lon_count - 1)

    to_hubs(send_sums)

    @pl.when(full)
    def _():
        send_edges()
        to_others(send_sums)
        pl.when(jnp.logical_not(first))(functools.partial(send_block, 0, whole))
        for peer, aside in others:
            pl.when(jnp.logical_and(peer >= HUB, aside))(functools.partial(send_block, peer, whole))
        pl.when(me != 1)(functools.partial(send_block, 1, whole))
        for peer, aside in others:
            pl.when(jnp.logical_and(peer >= HUB, jnp.logical_not(aside)))(functools.partial(send_block, peer, whole))

    @pl.when(early)
    def _():
        for pair in range(1, pair_count):
            pl.when(late)(functools.partial(send_block, 1, pl.ds(2 * pair, 2)))

        @pl.when(far)
        def _():
            send_block(1, whole)
            to_others(send_sums)
            to_others(send_block, whole)

        pl.semaphore_wait(go, 1)
        send_edges()

        @pl.when(late)
        def _():
            to_others(send_sums)
            to_others(send_block, whole)

    out_ref[:, :, :, my_lons] = send[:, pl.ds(me * own, own)]
    got[me] = sums[pl.ds(me * own, own + 2)]
    all_sums = got.at[pl.ds(0, lon_count - 1)]
    pltpu.make_async_copy(all_sums, all_sums, sum_recv.at[0]).wait()

    @pl.when(jnp.logical_or(jnp.logical_and(first, down), jnp.logical_and(last, up)))
    def _():
        pltpu.make_async_copy(cross, cross, edge_recv.at[0]).wait()

    def mean_of(parts):
        total = parts[0]
        for part in parts[1:]:
            total = total + part
        return total * (1 / count) if math.frexp(count)[0] == 0.5 else total / count

    here = [mean_of([got[l, j] for l in range(lon_count)]) for j in range(own + 2)]
    beyond_edge = mean_of([cross[l] for l in range(lon_count)])
    bottom = jnp.logical_and(first, band == 0)
    top = jnp.logical_and(last, band == lat_count - 1)
    for j in range(own):
        below, middle, above = here[j : j + 3]
        scale = jnp.float32(0.5)
        if j == 0:
            below = jnp.where(bottom, middle, jnp.where(first, beyond_edge, below))
            scale = jnp.where(bottom, 1.0, scale)
        if j == own - 1:
            above = jnp.where(top, middle, jnp.where(last, beyond_edge, above))
            scale = jnp.where(top, 1.0, scale)
        slope = scale * (above - below)
        for v in range(var_count):
            some = slice(v * plev_count, (v + 1) * plev_count)
            zonal[v, j : j + 1, :] = middle[:, some]
            merid[v, j : j + 1, :] = slope[:, some]

    pltpu.make_async_copy(all_sums, all_sums, sum_send.at[0]).wait()

    @pl.when(jnp.logical_and(up, down))
    def _():
        two = sums.at[pl.ds(0, 2)]
        pltpu.make_async_copy(two, two, edge_send.at[0]).wait()

    @pl.when(up != down)
    def _():
        one = sums.at[pl.ds(0, 1)]
        pltpu.make_async_copy(one, one, edge_send.at[0]).wait()

    landed = out_ref.at[:, :, :, pl.ds(0, (lon_count - 1) * lons)]
    pltpu.make_async_copy(landed, landed, recv_sem.at[0]).wait()
    left = send.at[:, pl.ds(0, row_count - own)]
    pltpu.make_async_copy(left, left, send_sem.at[0]).wait()


def finish(rows_vmem, zonal_vmem, merid_vmem, out_hbm, zonal_hbm, merid_hbm, sem):
    puts = [
        pltpu.make_async_copy(rows_vmem, out_hbm, sem.at[0]),
        pltpu.make_async_copy(zonal_vmem, zonal_hbm, sem.at[1]),
        pltpu.make_async_copy(merid_vmem, merid_hbm, sem.at[2]),
    ]
    for put in puts:
        put.start()
    for put in puts:
        put.wait()


def shards(lon_count, lat_count, fields, bracket, fraction):
    var_count, level_count, row_count, lons = fields.shape
    plev_count = bracket.shape[0]
    own = row_count // lon_count
    width = var_count * plev_count
    dma = pltpu.SemaphoreType.DMA
    anywhere = pl.BlockSpec(memory_space=pl.ANY)
    room = 2 * fields.size + 4 * bracket.size + 2 * fraction.size * (1 + var_count)
    in_vmem = pl.BlockSpec(memory_space=pltpu.VMEM)
    rows_shape = (var_count, own, plev_count, lons * lon_count)
    mean_shape = (var_count, own, plev_count)
    inputs = [pltpu.with_memory_space_constraint(x, pltpu.HBM) for x in (fields, bracket, fraction)]
    held = pl.pallas_call(
        functools.partial(exchange, lon_count, lat_count, float(lons * lon_count)),
        out_shape=(
            pltpu.VMEM(rows_shape, jnp.bfloat16),
            pltpu.VMEM(mean_shape, jnp.float32),
            pltpu.VMEM(mean_shape, jnp.float32),
        ),
        in_specs=[anywhere] * 3,
        out_specs=(in_vmem,) * 3,
        scratch_shapes=[
            pltpu.VMEM((var_count // 2, level_count, 2 * row_count, lons), fields.dtype),
            pltpu.VMEM(bracket.shape, bracket.dtype),
            pltpu.VMEM(fraction.shape, fraction.dtype),
            pltpu.VMEM((var_count, row_count, plev_count, lons), jnp.bfloat16),
            pltpu.VMEM((row_count + 2, 1, width), jnp.float32),
            pltpu.VMEM((lon_count, own + 2, 1, width), jnp.float32),
            pltpu.VMEM((lon_count, 1, width), jnp.float32),
            dma((2,)),
            dma((var_count // 2,)),
            dma((1,)),
            dma((1,)),
            dma((1,)),
            dma((1,)),
            dma((1,)),
            dma((1,)),
            pltpu.SemaphoreType.REGULAR,
        ],
        compiler_params=pltpu.CompilerParams(
            collective_id=0, has_side_effects=True, vmem_limit_bytes=room + (8 << 20)
        ),
    )(*inputs)
    held = [pltpu.with_memory_space_constraint(x, pltpu.VMEM) for x in held]
    on_pressure, zonal_mean, meridional = pl.pallas_call(
        finish,
        out_shape=(
            jax.ShapeDtypeStruct(rows_shape, jnp.bfloat16),
            jax.ShapeDtypeStruct(mean_shape, jnp.float32),
            jax.ShapeDtypeStruct(mean_shape, jnp.float32),
        ),
        in_specs=[in_vmem] * 3,
        out_specs=(anywhere,) * 3,
        scratch_shapes=[dma((3,))],
        compiler_params=pltpu.CompilerParams(vmem_limit_bytes=8 << 20),
    )(*held)
    return (
        on_pressure.transpose(0, 2, 1, 3),
        zonal_mean.transpose(0, 2, 1),
        meridional.transpose(0, 2, 1),
    )


def solution(mesh):
    return jax.shard_map(
        functools.partial(shards, mesh.shape["lon"], mesh.shape["lat"]),
        mesh=mesh,
        in_specs=(P(None, None, "lat", "lon"), P(None, "lat", "lon"), P(None, "lat", "lon")),
        out_specs=(
            P(None, None, ("lat", "lon"), None),
            P(None, None, ("lat", "lon")),
            P(None, None, ("lat", "lon")),
        ),
        check_vma=False,
    )
```

```python
import functools
import math

import jax
import jax.numpy as jnp
from jax import lax
from jax.experimental import pallas as pl
from jax.experimental.pallas import tpu as pltpu
from jax.sharding import PartitionSpec as P

WINDOW = 16
TILE = 8
PACK = 16
MESH = pl.DeviceIdType.MESH
HUB = 2
PARTS = (2, 2)


def select_pair(levels, masks):
    bit = len(levels) // 2
    for mask in masks:
        levels = [
            jnp.where(mask, levels[k + bit], levels[k]) if k + bit < len(levels) else levels[k]
            for k in range(bit + 1)
        ]
        bit //= 2
    return levels


def partner(me, k, count):
    if count & (count - 1):
        return (me + k) % count, (me + count - k) % count
    peer, bit = me, 1
    while bit < count:
        if k & bit:
            peer = peer + bit - 2 * bit * ((me // bit) % 2)
        bit *= 2
    return peer, peer


def interpolate(pair, levels, fields, bracket, fraction, send):
    _, level_count, both_rows, lons = fields.shape
    plev_count, row_count, _ = bracket.shape
    level_step = level_count // plev_count
    group_size = min(TILE, plev_count)

    def block(tile):
        where = [tile * PACK + half for half in range(0, PACK, TILE)]
        rows = [pl.ds(pl.multiple_of(at % row_count, TILE), TILE) for at in where]
        packed = pl.ds(pl.multiple_of(tile * PACK, PACK), PACK)
        loaded, groups = {}, [[], []]
        for p in levels:
            base = min(p * level_step, level_count - WINDOW)
            for k in range(base, base + WINDOW):
                if k not in loaded:
                    loaded[k] = fields[pair, k, packed, :]
            offset = (jnp.concatenate([bracket[p, r, :] for r in rows]) - base).astype(jnp.int16)
            masks, bit = [offset >= jnp.int16(WINDOW // 2)], WINDOW // 4
            while bit:
                masks.append((offset & jnp.int16(bit)) != jnp.int16(0))
                bit //= 2
            lower, upper = select_pair([loaded[base + k] for k in range(WINDOW)], masks)
            lower, upper = lower.astype(jnp.float32), upper.astype(jnp.float32)
            weight = jnp.concatenate([fraction[p, r, :].astype(jnp.float32) for r in rows])
            value = (lower + weight * (upper - lower)).astype(jnp.bfloat16)
            groups[0].append(value[:TILE])
            groups[1].append(value[TILE:])
            if len(groups[0]) == group_size:
                for half in range(2):
                    by_row = jnp.transpose(jnp.stack(groups[half]), (1, 0, 2))
                    v = 2 * pair + where[half] // row_count
                    send[v, rows[half], p + 1 - group_size : p + 1, :] = by_row
                groups = [[], []]

    if both_rows == PACK:
        block(0)
    else:
        pl.loop(0, both_rows // PACK)(block)


def exchange(
    lon_count, lat_count, count, fields_hbm, bracket_hbm, fraction_hbm,
    out_ref, zonal, merid,
    fields, bracket, fraction, send, sums, got, cross,
    in_sem, field_sem, send_sem, recv_sem, sum_recv, edge_recv, go,
):
    var_count, row_count, plev_count, lons = send.shape
    pair_count = var_count // 2
    own = row_count // lon_count
    width = var_count * plev_count
    me = lax.axis_index("lon")
    band = lax.axis_index("lat")
    next_band = (band + 1) % lat_count
    prev_band = (band + lat_count - 1) % lat_count
    first = me == 0
    last = me == lon_count - 1
    up = band < lat_count - 1
    down = band > 0
    my_lons = pl.ds(pl.multiple_of(me * lons, 128), lons)
    steps = range(lon_count - 1, 0, -1)
    peers = [partner(me, k, lon_count)[0] for k in steps]
    others = [(peer, (me // 2) % 2 != (k // 2) % 2) for k, peer in zip(steps, peers)]
    hub = me < HUB
    far = me >= lon_count - 2
    late = jnp.logical_and(me % 2 == 1, jnp.logical_not(jnp.logical_or(hub, far)))
    early = jnp.logical_or(far, late)
    full = jnp.logical_not(early)

    get_bracket = pltpu.make_async_copy(bracket_hbm, bracket, in_sem.at[0])
    get_fraction = pltpu.make_async_copy(fraction_hbm, fraction, in_sem.at[1])
    get_bracket.start()
    get_fraction.start()

    def get_pair(pair):
        for half in range(2):
            pltpu.make_async_copy(
                fields_hbm.at[2 * pair + half],
                fields.at[pair, :, pl.ds(half * row_count, row_count)],
                field_sem.at[pair],
            ).start()

    for pair in range(pair_count):
        get_pair(pair)

    barrier = pltpu.get_barrier_semaphore()

    def greet(peer, lat):
        pl.semaphore_signal(barrier, inc=1, device_id={"lon": peer, "lat": lat}, device_id_type=MESH)

    for peer in peers:
        listens = jnp.logical_or(jnp.logical_or(hub, peer % 2 == 0), jnp.logical_or(peer < HUB, peer >= lon_count - 2))
        pl.when(listens)(functools.partial(greet, peer, band))

    waiting = [l for l in range(lon_count - 2) if l < HUB or l % 2 == 0]

    @pl.when(jnp.logical_and(first, down))
    def _():
        for l in waiting:
            greet(l, prev_band)

    @pl.when(jnp.logical_and(last, up))
    def _():
        for l in waiting:
            greet(l, next_band)

    def send_block(peer, some, levels=slice(None)):
        pltpu.make_async_remote_copy(
            src_ref=send.at[some, pl.ds(peer * own, own), levels],
            dst_ref=out_ref.at[some, :, levels, my_lons],
            send_sem=send_sem.at[0],
            recv_sem=recv_sem.at[0],
            device_id={"lon": peer},
            device_id_type=MESH,
        ).start()

    def send_sums(peer):
        pltpu.make_async_remote_copy(
            src_ref=sums.at[pl.ds(peer * own, own + 2)],
            dst_ref=got.at[me],
            send_sem=send_sem.at[0],
            recv_sem=sum_recv.at[0],
            device_id={"lon": peer},
            device_id_type=MESH,
        ).start()

    def send_edge(row, lon, lat):
        pltpu.make_async_remote_copy(
            src_ref=sums.at[row],
            dst_ref=cross.at[me],
            send_sem=send_sem.at[0],
            recv_sem=edge_recv.at[0],
            device_id={"lon": lon, "lat": lat},
            device_id_type=MESH,
        ).start()

    def to_hubs(act, *args):
        for h in range(HUB):
            pl.when(me != h)(functools.partial(act, h, *args))

    def to_others(act, *args):
        for peer in peers:
            pl.when(peer >= HUB)(functools.partial(act, peer, *args))

    sums[0] = jnp.zeros((1, width), jnp.float32)
    sums[row_count + 1] = jnp.zeros((1, width), jnp.float32)
    get_bracket.wait()
    get_fraction.wait()
    whole = pl.ds(0, var_count)
    for pair in range(pair_count):
        pltpu.make_async_copy(fields.at[pair], fields.at[pair], field_sem.at[pair]).wait()
        some = pl.ds(2 * pair, 2)
        parts = PARTS[pair]
        for part in range(parts):
            count_here = plev_count // parts
            low = part * count_here
            interpolate(pair, range(low, low + count_here), fields, bracket, fraction, send)

            @pl.when(early)
            def _():
                if pair == 0 and part == 0:
                    pl.semaphore_wait(barrier, jnp.where(far, lon_count - 1, HUB))
                send_block(0, some, pl.ds(low, count_here))
                if pair == 0 and part == parts - 1:
                    pl.when(late)(functools.partial(send_block, 1, some))

    ones = jnp.ones((TILE, lons), jnp.bfloat16)

    def add_up(at):
        two = jnp.concatenate([send[:, at + r].reshape(width, lons) for r in range(2)])
        total = lax.dot_general(
            ones, two, (((1,), (1,)), ((), ())), preferred_element_type=jnp.float32
        )
        sums[at + 1] = total[0:1, :width]
        sums[at + 2] = total[0:1, width:]

    if row_count == TILE:
        for at in range(0, row_count, 2):
            add_up(at)
    else:
        pl.loop(0, row_count // 2)(lambda half: add_up(2 * half))

    def send_edges():
        pl.when(up)(lambda: send_edge(row_count, 0, next_band))
        pl.when(down)(lambda: send_edge(1, lon_count - 1, prev_band))

    def open_to(peer):
        pl.semaphore_signal(go, inc=1, device_id={"lon": peer}, device_id_type=MESH)

    @pl.when(full)
    def _():
        beyond = up.astype(jnp.int32) + down.astype(jnp.int32)
        pl.semaphore_wait(barrier, lon_count - 1 + beyond)
        pl.when(jnp.logical_not(hub))(lambda: open_to(me + 1))

        @pl.when(me == lon_count - 4)
        def _():
            open_to(lon_count - 2)
            open_to(lon_count - 1)

    to_hubs(send_sums)

    @pl.when(full)
    def _():
        send_edges()
        to_others(send_sums)
        pl.when(jnp.logical_not(first))(functools.partial(send_block, 0, whole))
        for peer, aside in others:
            pl.when(jnp.logical_and(peer >= HUB, aside))(functools.partial(send_block, peer, whole))
        pl.when(me != 1)(functools.partial(send_block, 1, whole))
        for peer, aside in others:
            pl.when(jnp.logical_and(peer >= HUB, jnp.logical_not(aside)))(functools.partial(send_block, peer, whole))

    @pl.when(early)
    def _():
        for pair in range(1, pair_count):
            pl.when(late)(functools.partial(send_block, 1, pl.ds(2 * pair, 2)))

        @pl.when(far)
        def _():
            send_block(1, whole)
            to_others(send_sums)
            to_others(send_block, whole)

        pl.semaphore_wait(go, 1)
        send_edges()

        @pl.when(late)
        def _():
            to_others(send_sums)
            to_others(send_block, whole)

    out_ref[:, :, :, my_lons] = send[:, pl.ds(me * own, own)]
    got[me] = sums[pl.ds(me * own, own + 2)]
    all_sums = got.at[pl.ds(0, lon_count - 1)]
    pltpu.make_async_copy(all_sums, all_sums, sum_recv.at[0]).wait()

    @pl.when(jnp.logical_or(jnp.logical_and(first, down), jnp.logical_and(last, up)))
    def _():
        pltpu.make_async_copy(cross, cross, edge_recv.at[0]).wait()

    def mean_of(parts):
        total = parts[0]
        for part in parts[1:]:
            total = total + part
        return total * (1 / count) if math.frexp(count)[0] == 0.5 else total / count

    here = [mean_of([got[l, j] for l in range(lon_count)]) for j in range(own + 2)]
    beyond_edge = mean_of([cross[l] for l in range(lon_count)])
    bottom = jnp.logical_and(first, band == 0)
    top = jnp.logical_and(last, band == lat_count - 1)
    for j in range(own):
        below, middle, above = here[j : j + 3]
        scale = jnp.float32(0.5)
        if j == 0:
            below = jnp.where(bottom, middle, jnp.where(first, beyond_edge, below))
            scale = jnp.where(bottom, 1.0, scale)
        if j == own - 1:
            above = jnp.where(top, middle, jnp.where(last, beyond_edge, above))
            scale = jnp.where(top, 1.0, scale)
        slope = scale * (above - below)
        for v in range(var_count):
            some = slice(v * plev_count, (v + 1) * plev_count)
            zonal[v, j : j + 1, :] = middle[:, some]
            merid[v, j : j + 1, :] = slope[:, some]

    pltpu.make_async_copy(all_sums, all_sums, send_sem.at[0]).wait()

    @pl.when(jnp.logical_and(up, down))
    def _():
        two = sums.at[pl.ds(0, 2)]
        pltpu.make_async_copy(two, two, send_sem.at[0]).wait()

    @pl.when(up != down)
    def _():
        one = sums.at[pl.ds(0, 1)]
        pltpu.make_async_copy(one, one, send_sem.at[0]).wait()

    landed = out_ref.at[:, :, :, pl.ds(0, (lon_count - 1) * lons)]
    pltpu.make_async_copy(landed, landed, recv_sem.at[0]).wait()
    left = send.at[:, pl.ds(0, row_count - own)]
    pltpu.make_async_copy(left, left, send_sem.at[0]).wait()


def finish(rows_vmem, zonal_vmem, merid_vmem, out_hbm, zonal_hbm, merid_hbm, sem):
    puts = [
        pltpu.make_async_copy(zonal_vmem, zonal_hbm, sem.at[1]),
        pltpu.make_async_copy(merid_vmem, merid_hbm, sem.at[2]),
    ]
    for v in range(rows_vmem.shape[0]):
        pltpu.make_async_copy(rows_vmem.at[v], out_hbm.at[v], sem.at[0]).start()
    for put in puts:
        put.start()
    for put in puts:
        put.wait()
    pltpu.make_async_copy(rows_vmem, out_hbm, sem.at[0]).wait()


def shards(lon_count, lat_count, fields, bracket, fraction):
    var_count, level_count, row_count, lons = fields.shape
    plev_count = bracket.shape[0]
    own = row_count // lon_count
    width = var_count * plev_count
    dma = pltpu.SemaphoreType.DMA
    anywhere = pl.BlockSpec(memory_space=pl.ANY)
    room = 2 * fields.size + 4 * bracket.size + 2 * fraction.size * (1 + var_count)
    in_vmem = pl.BlockSpec(memory_space=pltpu.VMEM)
    rows_shape = (var_count, own, plev_count, lons * lon_count)
    mean_shape = (var_count, own, plev_count)
    inputs = [pltpu.with_memory_space_constraint(x, pltpu.HBM) for x in (fields, bracket, fraction)]
    held = pl.pallas_call(
        functools.partial(exchange, lon_count, lat_count, float(lons * lon_count)),
        out_shape=(
            pltpu.VMEM(rows_shape, jnp.bfloat16),
            pltpu.VMEM(mean_shape, jnp.float32),
            pltpu.VMEM(mean_shape, jnp.float32),
        ),
        in_specs=[anywhere] * 3,
        out_specs=(in_vmem,) * 3,
        scratch_shapes=[
            pltpu.VMEM((var_count // 2, level_count, 2 * row_count, lons), fields.dtype),
            pltpu.VMEM(bracket.shape, bracket.dtype),
            pltpu.VMEM(fraction.shape, fraction.dtype),
            pltpu.VMEM((var_count, row_count, plev_count, lons), jnp.bfloat16),
            pltpu.VMEM((row_count + 2, 1, width), jnp.float32),
            pltpu.VMEM((lon_count, own + 2, 1, width), jnp.float32),
            pltpu.VMEM((lon_count, 1, width), jnp.float32),
            dma((2,)),
            dma((var_count // 2,)),
            dma((1,)),
            dma((1,)),
            dma((1,)),
            dma((1,)),
            pltpu.SemaphoreType.REGULAR,
        ],
        compiler_params=pltpu.CompilerParams(
            collective_id=0, has_side_effects=True, vmem_limit_bytes=room + (8 << 20)
        ),
    )(*inputs)
    held = [pltpu.with_memory_space_constraint(x, pltpu.VMEM) for x in held]
    on_pressure, zonal_mean, meridional = pl.pallas_call(
        finish,
        out_shape=(
            jax.ShapeDtypeStruct(rows_shape, jnp.bfloat16),
            jax.ShapeDtypeStruct(mean_shape, jnp.float32),
            jax.ShapeDtypeStruct(mean_shape, jnp.float32),
        ),
        in_specs=[in_vmem] * 3,
        out_specs=(anywhere,) * 3,
        scratch_shapes=[dma((3,))],
        compiler_params=pltpu.CompilerParams(vmem_limit_bytes=8 << 20),
    )(*held)
    return (
        on_pressure.transpose(0, 2, 1, 3),
        zonal_mean.transpose(0, 2, 1),
        meridional.transpose(0, 2, 1),
    )


def solution(mesh):
    return jax.shard_map(
        functools.partial(shards, mesh.shape["lon"], mesh.shape["lat"]),
        mesh=mesh,
        in_specs=(P(None, None, "lat", "lon"), P(None, "lat", "lon"), P(None, "lat", "lon")),
        out_specs=(
            P(None, None, ("lat", "lon"), None),
            P(None, None, ("lat", "lon")),
            P(None, None, ("lat", "lon")),
        ),
        check_vma=False,
    )
```

```python
import functools
import math

import jax
import jax.numpy as jnp
from jax import lax
from jax.experimental import pallas as pl
from jax.experimental.pallas import tpu as pltpu
from jax.sharding import PartitionSpec as P

WINDOW = 16
TILE = 8
PACK = 16
MESH = pl.DeviceIdType.MESH
HUB = 2
PARTS = (2, 2)


def select_pair(levels, masks):
    bit = len(levels) // 2
    for mask in masks:
        levels = [
            jnp.where(mask, levels[k + bit], levels[k]) if k + bit < len(levels) else levels[k]
            for k in range(bit + 1)
        ]
        bit //= 2
    return levels


def partner(me, k, count):
    if count & (count - 1):
        return (me + k) % count, (me + count - k) % count
    peer, bit = me, 1
    while bit < count:
        if k & bit:
            peer = peer + bit - 2 * bit * ((me // bit) % 2)
        bit *= 2
    return peer, peer


def interpolate(pair, levels, fields, bracket, fraction, send):
    _, level_count, both_rows, lons = fields.shape
    plev_count, row_count, _ = bracket.shape
    level_step = level_count // plev_count
    group_size = min(TILE, plev_count)

    def block(tile):
        where = [tile * PACK + half for half in range(0, PACK, TILE)]
        rows = [pl.ds(pl.multiple_of(at % row_count, TILE), TILE) for at in where]
        packed = pl.ds(pl.multiple_of(tile * PACK, PACK), PACK)
        loaded, groups = {}, [[], []]
        for p in levels:
            base = min(p * level_step, level_count - WINDOW)
            for k in range(base, base + WINDOW):
                if k not in loaded:
                    loaded[k] = fields[pair, k, packed, :]
            offset = (jnp.concatenate([bracket[p, r, :] for r in rows]) - base).astype(jnp.int16)
            masks, bit = [offset >= jnp.int16(WINDOW // 2)], WINDOW // 4
            while bit:
                masks.append((offset & jnp.int16(bit)) != jnp.int16(0))
                bit //= 2
            lower, upper = select_pair([loaded[base + k] for k in range(WINDOW)], masks)
            lower, upper = lower.astype(jnp.float32), upper.astype(jnp.float32)
            weight = jnp.concatenate([fraction[p, r, :].astype(jnp.float32) for r in rows])
            value = (lower + weight * (upper - lower)).astype(jnp.bfloat16)
            groups[0].append(value[:TILE])
            groups[1].append(value[TILE:])
            if len(groups[0]) == group_size:
                for half in range(2):
                    by_row = jnp.transpose(jnp.stack(groups[half]), (1, 0, 2))
                    v = 2 * pair + where[half] // row_count
                    send[v, rows[half], p + 1 - group_size : p + 1, :] = by_row
                groups = [[], []]

    if both_rows == PACK:
        block(0)
    else:
        pl.loop(0, both_rows // PACK)(block)


def exchange(
    lon_count, lat_count, count, fields_hbm, bracket_hbm, fraction_hbm,
    out_ref, zonal, merid,
    fields, bracket, fraction, send, sums, got, cross,
    in_sem, field_sem, send_sem, recv_sem, sum_recv, edge_recv, go,
):
    var_count, row_count, plev_count, lons = send.shape
    pair_count = var_count // 2
    own = row_count // lon_count
    width = var_count * plev_count
    me = lax.axis_index("lon")
    band = lax.axis_index("lat")
    next_band = (band + 1) % lat_count
    prev_band = (band + lat_count - 1) % lat_count
    first = me == 0
    last = me == lon_count - 1
    up = band < lat_count - 1
    down = band > 0
    my_lons = pl.ds(pl.multiple_of(me * lons, 128), lons)
    steps = range(lon_count - 1, 0, -1)
    peers = [partner(me, k, lon_count)[0] for k in steps]
    others = [(peer, (me // 2) % 2 != (k // 2) % 2) for k, peer in zip(steps, peers)]
    hub = me < HUB
    far = me >= lon_count - 2
    late = jnp.logical_and(me % 2 == 1, jnp.logical_not(jnp.logical_or(hub, far)))
    early = jnp.logical_or(far, late)
    full = jnp.logical_not(early)

    get_bracket = pltpu.make_async_copy(bracket_hbm, bracket, in_sem.at[0])
    get_fraction = pltpu.make_async_copy(fraction_hbm, fraction, in_sem.at[1])
    get_bracket.start()
    get_fraction.start()

    def get_pair(pair):
        for half in range(2):
            pltpu.make_async_copy(
                fields_hbm.at[2 * pair + half],
                fields.at[pair, :, pl.ds(half * row_count, row_count)],
                field_sem.at[pair],
            ).start()

    for pair in range(pair_count):
        get_pair(pair)

    barrier = pltpu.get_barrier_semaphore()

    def greet(peer, lat):
        pl.semaphore_signal(barrier, inc=1, device_id={"lon": peer, "lat": lat}, device_id_type=MESH)

    for peer in peers:
        listens = jnp.logical_or(jnp.logical_or(hub, peer % 2 == 0), jnp.logical_or(peer < HUB, peer >= lon_count - 2))
        apart = jnp.logical_and(far, peer < HUB)
        pl.when(jnp.logical_and(listens, jnp.logical_not(apart)))(functools.partial(greet, peer, band))

    waiting = [l for l in range(lon_count - 2) if l < HUB or l % 2 == 0]

    @pl.when(jnp.logical_and(first, down))
    def _():
        for l in waiting:
            greet(l, prev_band)

    @pl.when(jnp.logical_and(last, up))
    def _():
        for l in waiting:
            greet(l, next_band)

    def send_block(peer, some, levels=slice(None)):
        pltpu.make_async_remote_copy(
            src_ref=send.at[some, pl.ds(peer * own, own), levels],
            dst_ref=out_ref.at[some, :, levels, my_lons],
            send_sem=send_sem.at[0],
            recv_sem=recv_sem.at[0],
            device_id={"lon": peer},
            device_id_type=MESH,
        ).start()

    def send_sums(peer):
        pltpu.make_async_remote_copy(
            src_ref=sums.at[pl.ds(peer * own, own + 2)],
            dst_ref=got.at[me],
            send_sem=send_sem.at[0],
            recv_sem=sum_recv.at[0],
            device_id={"lon": peer},
            device_id_type=MESH,
        ).start()

    def send_edge(row, lon, lat):
        pltpu.make_async_remote_copy(
            src_ref=sums.at[row],
            dst_ref=cross.at[me],
            send_sem=send_sem.at[0],
            recv_sem=edge_recv.at[0],
            device_id={"lon": lon, "lat": lat},
            device_id_type=MESH,
        ).start()

    def to_hubs(act, *args):
        for h in range(HUB):
            pl.when(me != h)(functools.partial(act, h, *args))

    def to_others(act, *args):
        for peer in peers:
            pl.when(peer >= HUB)(functools.partial(act, peer, *args))

    def open_to(peer):
        pl.semaphore_signal(go, inc=1, device_id={"lon": peer}, device_id_type=MESH)

    @pl.when(far)
    def _():
        pl.semaphore_wait(barrier, lon_count - 1)
        for h in range(HUB):
            open_to(h)

    sums[0] = jnp.zeros((1, width), jnp.float32)
    sums[row_count + 1] = jnp.zeros((1, width), jnp.float32)
    get_bracket.wait()
    get_fraction.wait()
    whole = pl.ds(0, var_count)
    for pair in range(pair_count):
        pltpu.make_async_copy(fields.at[pair], fields.at[pair], field_sem.at[pair]).wait()
        some = pl.ds(2 * pair, 2)
        parts = PARTS[pair]
        for part in range(parts):
            count_here = plev_count // parts
            low = part * count_here
            interpolate(pair, range(low, low + count_here), fields, bracket, fraction, send)

            @pl.when(early)
            def _():
                if pair == 0 and part == 0:
                    pl.when(late)(lambda: pl.semaphore_wait(barrier, HUB))
                send_block(0, some, pl.ds(low, count_here))
                if pair == 0 and part == parts - 1:
                    pl.when(late)(functools.partial(send_block, 1, some))

    ones = jnp.ones((TILE, lons), jnp.bfloat16)

    def add_up(at):
        two = jnp.concatenate([send[:, at + r].reshape(width, lons) for r in range(2)])
        total = lax.dot_general(
            ones, two, (((1,), (1,)), ((), ())), preferred_element_type=jnp.float32
        )
        sums[at + 1] = total[0:1, :width]
        sums[at + 2] = total[0:1, width:]

    if row_count == TILE:
        for at in range(0, row_count, 2):
            add_up(at)
    else:
        pl.loop(0, row_count // 2)(lambda half: add_up(2 * half))

    def send_edges():
        pl.when(up)(lambda: send_edge(row_count, 0, next_band))
        pl.when(down)(lambda: send_edge(1, lon_count - 1, prev_band))

    beyond = up.astype(jnp.int32) + down.astype(jnp.int32)
    beside = jnp.logical_and(full, jnp.logical_not(hub))

    def choose(group, act, *args):
        for peer, aside in others:
            distant = peer >= lon_count - 2
            wanted = {
                "far": distant,
                "near": jnp.logical_not(jnp.logical_or(distant, peer < HUB)),
                "aside": jnp.logical_and(peer >= HUB, aside),
                "rest": jnp.logical_and(peer >= HUB, jnp.logical_not(aside)),
            }[group]
            pl.when(wanted)(functools.partial(act, peer, *args))

    def send_edges():
        pl.when(up)(lambda: send_edge(row_count, 0, next_band))
        pl.when(down)(lambda: send_edge(1, lon_count - 1, prev_band))

    @pl.when(hub)
    def _():
        pl.semaphore_wait(barrier, lon_count - 3 + beyond)
        choose("near", send_block, whole)
        to_hubs(send_sums)
        choose("near", send_sums)
        pl.when(me == 1)(functools.partial(send_block, 0, whole))
        pl.when(me == 0)(functools.partial(send_block, 1, whole))
        pl.semaphore_wait(go, 2)
        send_edges()
        choose("far", send_sums)
        choose("far", send_block, whole)

    @pl.when(beside)
    def _():
        pl.semaphore_wait(barrier, lon_count - 1 + beyond)
        open_to(me + 1)

        @pl.when(me == lon_count - 4)
        def _():
            open_to(lon_count - 2)
            open_to(lon_count - 1)

        to_hubs(send_sums)
        send_edges()
        to_others(send_sums)
        send_block(0, whole)
        choose("aside", send_block, whole)
        send_block(1, whole)
        choose("rest", send_block, whole)

    @pl.when(early)
    def _():
        to_hubs(send_sums)
        for pair in range(1, pair_count):
            pl.when(late)(functools.partial(send_block, 1, pl.ds(2 * pair, 2)))

        @pl.when(far)
        def _():
            send_block(1, whole)
            to_others(send_sums)
            to_others(send_block, whole)

        pl.semaphore_wait(go, 1)
        send_edges()

        @pl.when(late)
        def _():
            to_others(send_sums)
            to_others(send_block, whole)

    out_ref[:, :, :, my_lons] = send[:, pl.ds(me * own, own)]
    got[me] = sums[pl.ds(me * own, own + 2)]
    all_sums = got.at[pl.ds(0, lon_count - 1)]
    pltpu.make_async_copy(all_sums, all_sums, sum_recv.at[0]).wait()

    @pl.when(jnp.logical_or(jnp.logical_and(first, down), jnp.logical_and(last, up)))
    def _():
        pltpu.make_async_copy(cross, cross, edge_recv.at[0]).wait()

    def mean_of(parts):
        total = parts[0]
        for part in parts[1:]:
            total = total + part
        return total * (1 / count) if math.frexp(count)[0] == 0.5 else total / count

    here = [mean_of([got[l, j] for l in range(lon_count)]) for j in range(own + 2)]
    beyond_edge = mean_of([cross[l] for l in range(lon_count)])
    bottom = jnp.logical_and(first, band == 0)
    top = jnp.logical_and(last, band == lat_count - 1)
    for j in range(own):
        below, middle, above = here[j : j + 3]
        scale = jnp.float32(0.5)
        if j == 0:
            below = jnp.where(bottom, middle, jnp.where(first, beyond_edge, below))
            scale = jnp.where(bottom, 1.0, scale)
        if j == own - 1:
            above = jnp.where(top, middle, jnp.where(last, beyond_edge, above))
            scale = jnp.where(top, 1.0, scale)
        slope = scale * (above - below)
        for v in range(var_count):
            some = slice(v * plev_count, (v + 1) * plev_count)
            zonal[v, j : j + 1, :] = middle[:, some]
            merid[v, j : j + 1, :] = slope[:, some]

    pltpu.make_async_copy(all_sums, all_sums, send_sem.at[0]).wait()

    @pl.when(jnp.logical_and(up, down))
    def _():
        two = sums.at[pl.ds(0, 2)]
        pltpu.make_async_copy(two, two, send_sem.at[0]).wait()

    @pl.when(up != down)
    def _():
        one = sums.at[pl.ds(0, 1)]
        pltpu.make_async_copy(one, one, send_sem.at[0]).wait()

    landed = out_ref.at[:, :, :, pl.ds(0, (lon_count - 1) * lons)]
    pltpu.make_async_copy(landed, landed, recv_sem.at[0]).wait()
    left = send.at[:, pl.ds(0, row_count - own)]
    pltpu.make_async_copy(left, left, send_sem.at[0]).wait()


def finish(rows_vmem, zonal_vmem, merid_vmem, out_hbm, zonal_hbm, merid_hbm, sem):
    puts = [
        pltpu.make_async_copy(zonal_vmem, zonal_hbm, sem.at[1]),
        pltpu.make_async_copy(merid_vmem, merid_hbm, sem.at[2]),
    ]
    for v in range(rows_vmem.shape[0]):
        pltpu.make_async_copy(rows_vmem.at[v], out_hbm.at[v], sem.at[0]).start()
    for put in puts:
        put.start()
    for put in puts:
        put.wait()
    pltpu.make_async_copy(rows_vmem, out_hbm, sem.at[0]).wait()


def shards(lon_count, lat_count, fields, bracket, fraction):
    var_count, level_count, row_count, lons = fields.shape
    plev_count = bracket.shape[0]
    own = row_count // lon_count
    width = var_count * plev_count
    dma = pltpu.SemaphoreType.DMA
    anywhere = pl.BlockSpec(memory_space=pl.ANY)
    room = 2 * fields.size + 4 * bracket.size + 2 * fraction.size * (1 + var_count)
    in_vmem = pl.BlockSpec(memory_space=pltpu.VMEM)
    rows_shape = (var_count, own, plev_count, lons * lon_count)
    mean_shape = (var_count, own, plev_count)
    inputs = [pltpu.with_memory_space_constraint(x, pltpu.HBM) for x in (fields, bracket, fraction)]
    held = pl.pallas_call(
        functools.partial(exchange, lon_count, lat_count, float(lons * lon_count)),
        out_shape=(
            pltpu.VMEM(rows_shape, jnp.bfloat16),
            pltpu.VMEM(mean_shape, jnp.float32),
            pltpu.VMEM(mean_shape, jnp.float32),
        ),
        in_specs=[anywhere] * 3,
        out_specs=(in_vmem,) * 3,
        scratch_shapes=[
            pltpu.VMEM((var_count // 2, level_count, 2 * row_count, lons), fields.dtype),
            pltpu.VMEM(bracket.shape, bracket.dtype),
            pltpu.VMEM(fraction.shape, fraction.dtype),
            pltpu.VMEM((var_count, row_count, plev_count, lons), jnp.bfloat16),
            pltpu.VMEM((row_count + 2, 1, width), jnp.float32),
            pltpu.VMEM((lon_count, own + 2, 1, width), jnp.float32),
            pltpu.VMEM((lon_count, 1, width), jnp.float32),
            dma((2,)),
            dma((var_count // 2,)),
            dma((1,)),
            dma((1,)),
            dma((1,)),
            dma((1,)),
            pltpu.SemaphoreType.REGULAR,
        ],
        compiler_params=pltpu.CompilerParams(
            collective_id=0, has_side_effects=True, vmem_limit_bytes=room + (8 << 20)
        ),
    )(*inputs)
    held = [pltpu.with_memory_space_constraint(x, pltpu.VMEM) for x in held]
    on_pressure, zonal_mean, meridional = pl.pallas_call(
        finish,
        out_shape=(
            jax.ShapeDtypeStruct(rows_shape, jnp.bfloat16),
            jax.ShapeDtypeStruct(mean_shape, jnp.float32),
            jax.ShapeDtypeStruct(mean_shape, jnp.float32),
        ),
        in_specs=[in_vmem] * 3,
        out_specs=(anywhere,) * 3,
        scratch_shapes=[dma((3,))],
        compiler_params=pltpu.CompilerParams(vmem_limit_bytes=8 << 20),
    )(*held)
    return (
        on_pressure.transpose(0, 2, 1, 3),
        zonal_mean.transpose(0, 2, 1),
        meridional.transpose(0, 2, 1),
    )


def solution(mesh):
    return jax.shard_map(
        functools.partial(shards, mesh.shape["lon"], mesh.shape["lat"]),
        mesh=mesh,
        in_specs=(P(None, None, "lat", "lon"), P(None, "lat", "lon"), P(None, "lat", "lon")),
        out_specs=(
            P(None, None, ("lat", "lon"), None),
            P(None, None, ("lat", "lon")),
            P(None, None, ("lat", "lon")),
        ),
        check_vma=False,
    )
```

```python
import functools
import math

import jax
import jax.numpy as jnp
from jax import lax
from jax.experimental import pallas as pl
from jax.experimental.pallas import tpu as pltpu
from jax.sharding import PartitionSpec as P

WINDOW = 16
TILE = 8
PACK = 16
MESH = pl.DeviceIdType.MESH
HUB = 2
PARTS = (2, 2)


def select_pair(levels, masks):
    bit = len(levels) // 2
    for mask in masks:
        levels = [
            jnp.where(mask, levels[k + bit], levels[k]) if k + bit < len(levels) else levels[k]
            for k in range(bit + 1)
        ]
        bit //= 2
    return levels


def partner(me, k, count):
    if count & (count - 1):
        return (me + k) % count, (me + count - k) % count
    peer, bit = me, 1
    while bit < count:
        if k & bit:
            peer = peer + bit - 2 * bit * ((me // bit) % 2)
        bit *= 2
    return peer, peer


def interpolate(pair, levels, fields, bracket, fraction, send):
    _, level_count, both_rows, lons = fields.shape
    plev_count, row_count, _ = bracket.shape
    level_step = level_count // plev_count
    group_size = min(TILE, plev_count)

    def block(tile):
        where = [tile * PACK + half for half in range(0, PACK, TILE)]
        rows = [pl.ds(pl.multiple_of(at % row_count, TILE), TILE) for at in where]
        packed = pl.ds(pl.multiple_of(tile * PACK, PACK), PACK)
        loaded, groups = {}, [[], []]
        for p in levels:
            base = min(p * level_step, level_count - WINDOW)
            for k in range(base, base + WINDOW):
                if k not in loaded:
                    loaded[k] = fields[pair, k, packed, :]
            offset = (jnp.concatenate([bracket[p, r, :] for r in rows]) - base).astype(jnp.int16)
            masks, bit = [offset >= jnp.int16(WINDOW // 2)], WINDOW // 4
            while bit:
                masks.append((offset & jnp.int16(bit)) != jnp.int16(0))
                bit //= 2
            lower, upper = select_pair([loaded[base + k] for k in range(WINDOW)], masks)
            lower, upper = lower.astype(jnp.float32), upper.astype(jnp.float32)
            weight = jnp.concatenate([fraction[p, r, :].astype(jnp.float32) for r in rows])
            value = (lower + weight * (upper - lower)).astype(jnp.bfloat16)
            groups[0].append(value[:TILE])
            groups[1].append(value[TILE:])
            if len(groups[0]) == group_size:
                for half in range(2):
                    by_row = jnp.transpose(jnp.stack(groups[half]), (1, 0, 2))
                    v = 2 * pair + where[half] // row_count
                    send[v, rows[half], p + 1 - group_size : p + 1, :] = by_row
                groups = [[], []]

    if both_rows == PACK:
        block(0)
    else:
        pl.loop(0, both_rows // PACK)(block)


def exchange(
    lon_count, lat_count, count, fields_hbm, bracket_hbm, fraction_hbm,
    out_ref, zonal, merid,
    fields, bracket, fraction, send, sums, got, cross,
    in_sem, field_sem, send_sem, recv_sem, sum_recv, edge_recv, go,
):
    var_count, row_count, plev_count, lons = send.shape
    pair_count = var_count // 2
    own = row_count // lon_count
    width = var_count * plev_count
    me = lax.axis_index("lon")
    band = lax.axis_index("lat")
    next_band = (band + 1) % lat_count
    prev_band = (band + lat_count - 1) % lat_count
    first = me == 0
    last = me == lon_count - 1
    up = band < lat_count - 1
    down = band > 0
    my_lons = pl.ds(pl.multiple_of(me * lons, 128), lons)
    steps = range(lon_count - 1, 0, -1)
    peers = [partner(me, k, lon_count)[0] for k in steps]
    others = [(peer, (me // 2) % 2 != (k // 2) % 2) for k, peer in zip(steps, peers)]
    hub = me < HUB
    far = me >= lon_count - 2
    late = jnp.logical_and(me % 2 == 1, jnp.logical_not(jnp.logical_or(hub, far)))
    early = jnp.logical_or(far, late)
    full = jnp.logical_not(early)

    get_bracket = pltpu.make_async_copy(bracket_hbm, bracket, in_sem.at[0])
    get_fraction = pltpu.make_async_copy(fraction_hbm, fraction, in_sem.at[1])
    get_bracket.start()
    get_fraction.start()

    def get_pair(pair):
        for half in range(2):
            pltpu.make_async_copy(
                fields_hbm.at[2 * pair + half],
                fields.at[pair, :, pl.ds(half * row_count, row_count)],
                field_sem.at[pair],
            ).start()

    for pair in range(pair_count):
        get_pair(pair)

    barrier = pltpu.get_barrier_semaphore()

    def greet(peer, lat):
        pl.semaphore_signal(barrier, inc=1, device_id={"lon": peer, "lat": lat}, device_id_type=MESH)

    for peer in peers:
        listens = jnp.logical_or(jnp.logical_or(hub, peer % 2 == 0), jnp.logical_or(peer < HUB, peer >= lon_count - 2))
        apart = jnp.logical_and(far, peer < HUB)
        pl.when(jnp.logical_and(listens, jnp.logical_not(apart)))(functools.partial(greet, peer, band))

    waiting = [l for l in range(lon_count - 2) if l < HUB or l % 2 == 0]

    @pl.when(jnp.logical_and(first, down))
    def _():
        for l in waiting:
            greet(l, prev_band)

    @pl.when(jnp.logical_and(last, up))
    def _():
        for l in waiting:
            greet(l, next_band)

    def send_block(peer, some, levels=slice(None)):
        pltpu.make_async_remote_copy(
            src_ref=send.at[some, pl.ds(peer * own, own), levels],
            dst_ref=out_ref.at[some, :, levels, my_lons],
            send_sem=send_sem.at[0],
            recv_sem=recv_sem.at[0],
            device_id={"lon": peer},
            device_id_type=MESH,
        ).start()

    def send_sums(peer):
        pltpu.make_async_remote_copy(
            src_ref=sums.at[pl.ds(peer * own, own + 2)],
            dst_ref=got.at[me],
            send_sem=send_sem.at[0],
            recv_sem=sum_recv.at[0],
            device_id={"lon": peer},
            device_id_type=MESH,
        ).start()

    def send_edge(row, lon, lat):
        pltpu.make_async_remote_copy(
            src_ref=sums.at[row],
            dst_ref=cross.at[me],
            send_sem=send_sem.at[0],
            recv_sem=edge_recv.at[0],
            device_id={"lon": lon, "lat": lat},
            device_id_type=MESH,
        ).start()

    def to_hubs(act, *args):
        for h in range(HUB):
            pl.when(me != h)(functools.partial(act, h, *args))

    def to_others(act, *args):
        for peer in peers:
            pl.when(peer >= HUB)(functools.partial(act, peer, *args))

    def open_to(peer):
        pl.semaphore_signal(go, inc=1, device_id={"lon": peer}, device_id_type=MESH)

    @pl.when(far)
    def _():
        pl.semaphore_wait(barrier, lon_count - 1)
        for h in range(HUB):
            open_to(h)

    sums[0] = jnp.zeros((1, width), jnp.float32)
    sums[row_count + 1] = jnp.zeros((1, width), jnp.float32)
    get_bracket.wait()
    get_fraction.wait()
    whole = pl.ds(0, var_count)
    for pair in range(pair_count):
        pltpu.make_async_copy(fields.at[pair], fields.at[pair], field_sem.at[pair]).wait()
        some = pl.ds(2 * pair, 2)
        parts = PARTS[pair]
        for part in range(parts):
            count_here = plev_count // parts
            low = part * count_here
            interpolate(pair, range(low, low + count_here), fields, bracket, fraction, send)

            if pair == pair_count - 1 and part == parts - 1:
                continue

            @pl.when(early)
            def _():
                if pair == 0 and part == 0:
                    pl.when(late)(lambda: pl.semaphore_wait(barrier, HUB))
                send_block(0, some, pl.ds(low, count_here))
                if pair == 0 and part == parts - 1:
                    pl.when(jnp.logical_or(late, last))(functools.partial(send_block, 1, some))

    ones = jnp.ones((TILE, lons), jnp.bfloat16)

    def add_up(at):
        two = jnp.concatenate([send[:, at + r].reshape(width, lons) for r in range(2)])
        total = lax.dot_general(
            ones, two, (((1,), (1,)), ((), ())), preferred_element_type=jnp.float32
        )
        sums[at + 1] = total[0:1, :width]
        sums[at + 2] = total[0:1, width:]

    if row_count == TILE:
        for at in range(0, row_count, 2):
            add_up(at)
    else:
        pl.loop(0, row_count // 2)(lambda half: add_up(2 * half))

    def send_edges():
        pl.when(up)(lambda: send_edge(row_count, 0, next_band))
        pl.when(down)(lambda: send_edge(1, lon_count - 1, prev_band))

    beyond = up.astype(jnp.int32) + down.astype(jnp.int32)
    beside = jnp.logical_and(full, jnp.logical_not(hub))

    def choose(group, act, *args):
        for peer, aside in others:
            distant = peer >= lon_count - 2
            wanted = {
                "far": distant,
                "near": jnp.logical_not(jnp.logical_or(distant, peer < HUB)),
                "aside": jnp.logical_and(peer >= HUB, aside),
                "rest": jnp.logical_and(peer >= HUB, jnp.logical_not(aside)),
            }[group]
            pl.when(wanted)(functools.partial(act, peer, *args))

    def send_edges():
        pl.when(up)(lambda: send_edge(row_count, 0, next_band))
        pl.when(down)(lambda: send_edge(1, lon_count - 1, prev_band))

    @pl.when(hub)
    def _():
        pl.semaphore_wait(barrier, lon_count - 3 + beyond)
        choose("near", send_block, whole)
        to_hubs(send_sums)
        choose("near", send_sums)
        pl.when(me == 1)(functools.partial(send_block, 0, whole))
        pl.when(me == 0)(functools.partial(send_block, 1, whole))
        pl.semaphore_wait(go, 2)
        send_edges()
        choose("far", send_sums)
        choose("far", send_block, whole)

    @pl.when(beside)
    def _():
        pl.semaphore_wait(barrier, lon_count - 1 + beyond)
        open_to(me + 1)

        @pl.when(me == lon_count - 4)
        def _():
            open_to(lon_count - 2)
            open_to(lon_count - 1)

        to_hubs(send_sums)
        send_edges()
        to_others(send_sums)
        send_block(0, whole)
        choose("aside", send_block, whole)
        send_block(1, whole)
        choose("rest", send_block, whole)

    @pl.when(early)
    def _():
        send_sums(0)
        send_block(0, some, pl.ds(low, count_here))
        send_sums(1)
        for pair in range(1, pair_count):
            pl.when(late)(functools.partial(send_block, 1, pl.ds(2 * pair, 2)))

        @pl.when(far)
        def _():
            pl.when(last)(functools.partial(send_block, 1, pl.ds(2, var_count - 2)))
            pl.when(jnp.logical_not(last))(functools.partial(send_block, 1, whole))
            to_others(send_sums)
            to_others(send_block, whole)

        pl.semaphore_wait(go, 1)
        send_edges()

        @pl.when(late)
        def _():
            to_others(send_sums)
            to_others(send_block, whole)

    out_ref[:, :, :, my_lons] = send[:, pl.ds(me * own, own)]
    got[me] = sums[pl.ds(me * own, own + 2)]
    all_sums = got.at[pl.ds(0, lon_count - 1)]
    pltpu.make_async_copy(all_sums, all_sums, sum_recv.at[0]).wait()

    @pl.when(jnp.logical_or(jnp.logical_and(first, down), jnp.logical_and(last, up)))
    def _():
        pltpu.make_async_copy(cross, cross, edge_recv.at[0]).wait()

    def mean_of(parts):
        total = parts[0]
        for part in parts[1:]:
            total = total + part
        return total * (1 / count) if math.frexp(count)[0] == 0.5 else total / count

    here = [mean_of([got[l, j] for l in range(lon_count)]) for j in range(own + 2)]
    beyond_edge = mean_of([cross[l] for l in range(lon_count)])
    bottom = jnp.logical_and(first, band == 0)
    top = jnp.logical_and(last, band == lat_count - 1)
    for j in range(own):
        below, middle, above = here[j : j + 3]
        scale = jnp.float32(0.5)
        if j == 0:
            below = jnp.where(bottom, middle, jnp.where(first, beyond_edge, below))
            scale = jnp.where(bottom, 1.0, scale)
        if j == own - 1:
            above = jnp.where(top, middle, jnp.where(last, beyond_edge, above))
            scale = jnp.where(top, 1.0, scale)
        slope = scale * (above - below)
        for v in range(var_count):
            some = slice(v * plev_count, (v + 1) * plev_count)
            zonal[v, j : j + 1, :] = middle[:, some]
            merid[v, j : j + 1, :] = slope[:, some]

    pltpu.make_async_copy(all_sums, all_sums, send_sem.at[0]).wait()

    @pl.when(jnp.logical_and(up, down))
    def _():
        two = sums.at[pl.ds(0, 2)]
        pltpu.make_async_copy(two, two, send_sem.at[0]).wait()

    @pl.when(up != down)
    def _():
        one = sums.at[pl.ds(0, 1)]
        pltpu.make_async_copy(one, one, send_sem.at[0]).wait()

    landed = out_ref.at[:, :, :, pl.ds(0, (lon_count - 1) * lons)]
    pltpu.make_async_copy(landed, landed, recv_sem.at[0]).wait()
    left = send.at[:, pl.ds(0, row_count - own)]
    pltpu.make_async_copy(left, left, send_sem.at[0]).wait()


def finish(rows_vmem, zonal_vmem, merid_vmem, out_hbm, zonal_hbm, merid_hbm, sem):
    puts = [
        pltpu.make_async_copy(zonal_vmem, zonal_hbm, sem.at[1]),
        pltpu.make_async_copy(merid_vmem, merid_hbm, sem.at[2]),
    ]
    for v in range(rows_vmem.shape[0]):
        pltpu.make_async_copy(rows_vmem.at[v], out_hbm.at[v], sem.at[0]).start()
    for put in puts:
        put.start()
    for put in puts:
        put.wait()
    pltpu.make_async_copy(rows_vmem, out_hbm, sem.at[0]).wait()


def shards(lon_count, lat_count, fields, bracket, fraction):
    var_count, level_count, row_count, lons = fields.shape
    plev_count = bracket.shape[0]
    own = row_count // lon_count
    width = var_count * plev_count
    dma = pltpu.SemaphoreType.DMA
    anywhere = pl.BlockSpec(memory_space=pl.ANY)
    room = 2 * fields.size + 4 * bracket.size + 2 * fraction.size * (1 + var_count)
    in_vmem = pl.BlockSpec(memory_space=pltpu.VMEM)
    rows_shape = (var_count, own, plev_count, lons * lon_count)
    mean_shape = (var_count, own, plev_count)
    inputs = [pltpu.with_memory_space_constraint(x, pltpu.HBM) for x in (fields, bracket, fraction)]
    held = pl.pallas_call(
        functools.partial(exchange, lon_count, lat_count, float(lons * lon_count)),
        out_shape=(
            pltpu.VMEM(rows_shape, jnp.bfloat16),
            pltpu.VMEM(mean_shape, jnp.float32),
            pltpu.VMEM(mean_shape, jnp.float32),
        ),
        in_specs=[anywhere] * 3,
        out_specs=(in_vmem,) * 3,
        scratch_shapes=[
            pltpu.VMEM((var_count // 2, level_count, 2 * row_count, lons), fields.dtype),
            pltpu.VMEM(bracket.shape, bracket.dtype),
            pltpu.VMEM(fraction.shape, fraction.dtype),
            pltpu.VMEM((var_count, row_count, plev_count, lons), jnp.bfloat16),
            pltpu.VMEM((row_count + 2, 1, width), jnp.float32),
            pltpu.VMEM((lon_count, own + 2, 1, width), jnp.float32),
            pltpu.VMEM((lon_count, 1, width), jnp.float32),
            dma((2,)),
            dma((var_count // 2,)),
            dma((1,)),
            dma((1,)),
            dma((1,)),
            dma((1,)),
            pltpu.SemaphoreType.REGULAR,
        ],
        compiler_params=pltpu.CompilerParams(
            collective_id=0, has_side_effects=True, vmem_limit_bytes=room + (8 << 20)
        ),
    )(*inputs)
    held = [pltpu.with_memory_space_constraint(x, pltpu.VMEM) for x in held]
    on_pressure, zonal_mean, meridional = pl.pallas_call(
        finish,
        out_shape=(
            jax.ShapeDtypeStruct(rows_shape, jnp.bfloat16),
            jax.ShapeDtypeStruct(mean_shape, jnp.float32),
            jax.ShapeDtypeStruct(mean_shape, jnp.float32),
        ),
        in_specs=[in_vmem] * 3,
        out_specs=(anywhere,) * 3,
        scratch_shapes=[dma((3,))],
        compiler_params=pltpu.CompilerParams(vmem_limit_bytes=8 << 20),
    )(*held)
    return (
        on_pressure.transpose(0, 2, 1, 3),
        zonal_mean.transpose(0, 2, 1),
        meridional.transpose(0, 2, 1),
    )


def solution(mesh):
    return jax.shard_map(
        functools.partial(shards, mesh.shape["lon"], mesh.shape["lat"]),
        mesh=mesh,
        in_specs=(P(None, None, "lat", "lon"), P(None, "lat", "lon"), P(None, "lat", "lon")),
        out_specs=(
            P(None, None, ("lat", "lon"), None),
            P(None, None, ("lat", "lon")),
            P(None, None, ("lat", "lon")),
        ),
        check_vma=False,
    )
```

```python
import functools
import math

import jax
import jax.numpy as jnp
from jax import lax
from jax.experimental import pallas as pl
from jax.experimental.pallas import tpu as pltpu
from jax.sharding import PartitionSpec as P

WINDOW = 16
TILE = 8
PACK = 16
MESH = pl.DeviceIdType.MESH
HUB = 2
PARTS = (2, 2)


def select_pair(levels, masks):
    bit = len(levels) // 2
    for mask in masks:
        levels = [
            jnp.where(mask, levels[k + bit], levels[k]) if k + bit < len(levels) else levels[k]
            for k in range(bit + 1)
        ]
        bit //= 2
    return levels


def partner(me, k, count):
    if count & (count - 1):
        return (me + k) % count, (me + count - k) % count
    peer, bit = me, 1
    while bit < count:
        if k & bit:
            peer = peer + bit - 2 * bit * ((me // bit) % 2)
        bit *= 2
    return peer, peer


def interpolate(pair, levels, fields, bracket, fraction, send):
    _, level_count, both_rows, lons = fields.shape
    plev_count, row_count, _ = bracket.shape
    level_step = level_count // plev_count
    group_size = min(TILE, plev_count)

    def block(tile):
        where = [tile * PACK + half for half in range(0, PACK, TILE)]
        rows = [pl.ds(pl.multiple_of(at % row_count, TILE), TILE) for at in where]
        packed = pl.ds(pl.multiple_of(tile * PACK, PACK), PACK)
        loaded, groups = {}, [[], []]
        for p in levels:
            base = min(p * level_step, level_count - WINDOW)
            for k in range(base, base + WINDOW):
                if k not in loaded:
                    loaded[k] = fields[pair, k, packed, :]
            offset = (jnp.concatenate([bracket[p, r, :] for r in rows]) - base).astype(jnp.int16)
            masks, bit = [offset >= jnp.int16(WINDOW // 2)], WINDOW // 4
            while bit:
                masks.append((offset & jnp.int16(bit)) != jnp.int16(0))
                bit //= 2
            lower, upper = select_pair([loaded[base + k] for k in range(WINDOW)], masks)
            lower, upper = lower.astype(jnp.float32), upper.astype(jnp.float32)
            weight = jnp.concatenate([fraction[p, r, :].astype(jnp.float32) for r in rows])
            value = (lower + weight * (upper - lower)).astype(jnp.bfloat16)
            groups[0].append(value[:TILE])
            groups[1].append(value[TILE:])
            if len(groups[0]) == group_size:
                for half in range(2):
                    by_row = jnp.transpose(jnp.stack(groups[half]), (1, 0, 2))
                    v = 2 * pair + where[half] // row_count
                    send[v, rows[half], p + 1 - group_size : p + 1, :] = by_row
                groups = [[], []]

    if both_rows == PACK:
        block(0)
    else:
        pl.loop(0, both_rows // PACK)(block)


def exchange(
    lon_count, lat_count, count, fields_hbm, bracket_hbm, fraction_hbm,
    out_ref, zonal, merid,
    fields, bracket, fraction, send, sums, got, cross,
    in_sem, field_sem, send_sem, recv_sem, sum_recv, edge_recv, go,
):
    var_count, row_count, plev_count, lons = send.shape
    pair_count = var_count // 2
    own = row_count // lon_count
    width = var_count * plev_count
    me = lax.axis_index("lon")
    band = lax.axis_index("lat")
    next_band = (band + 1) % lat_count
    prev_band = (band + lat_count - 1) % lat_count
    first = me == 0
    last = me == lon_count - 1
    up = band < lat_count - 1
    down = band > 0
    my_lons = pl.ds(pl.multiple_of(me * lons, 128), lons)
    steps = range(lon_count - 1, 0, -1)
    peers = [partner(me, k, lon_count)[0] for k in steps]
    others = [(peer, (me // 2) % 2 != (k // 2) % 2) for k, peer in zip(steps, peers)]
    hub = me < HUB
    far = me >= lon_count - 2
    late = jnp.logical_and(me % 2 == 1, jnp.logical_not(jnp.logical_or(hub, far)))
    early = jnp.logical_or(far, late)
    full = jnp.logical_not(early)

    get_bracket = pltpu.make_async_copy(bracket_hbm, bracket, in_sem.at[0])
    get_fraction = pltpu.make_async_copy(fraction_hbm, fraction, in_sem.at[0])
    get_bracket.start()
    get_fraction.start()

    def get_pair(pair):
        for half in range(2):
            pltpu.make_async_copy(
                fields_hbm.at[2 * pair + half],
                fields.at[pair, :, pl.ds(half * row_count, row_count)],
                field_sem.at[pair],
            ).start()

    for pair in range(pair_count):
        get_pair(pair)

    barrier = pltpu.get_barrier_semaphore()

    def greet(peer, lat):
        pl.semaphore_signal(barrier, inc=1, device_id={"lon": peer, "lat": lat}, device_id_type=MESH)

    for peer in peers:
        listens = jnp.logical_or(jnp.logical_or(hub, peer % 2 == 0), jnp.logical_or(peer < HUB, peer >= lon_count - 2))
        apart = jnp.logical_and(far, peer < HUB)
        pl.when(jnp.logical_and(listens, jnp.logical_not(apart)))(functools.partial(greet, peer, band))

    waiting = [l for l in range(lon_count - 2) if l < HUB or l % 2 == 0]

    @pl.when(jnp.logical_and(first, down))
    def _():
        for l in waiting:
            greet(l, prev_band)

    @pl.when(jnp.logical_and(last, up))
    def _():
        for l in waiting:
            greet(l, next_band)

    def send_block(peer, some, levels=slice(None)):
        pltpu.make_async_remote_copy(
            src_ref=send.at[some, pl.ds(peer * own, own), levels],
            dst_ref=out_ref.at[some, :, levels, my_lons],
            send_sem=send_sem.at[0],
            recv_sem=recv_sem.at[0],
            device_id={"lon": peer},
            device_id_type=MESH,
        ).start()

    def send_sums(peer):
        pltpu.make_async_remote_copy(
            src_ref=sums.at[pl.ds(peer * own, own + 2)],
            dst_ref=got.at[me],
            send_sem=send_sem.at[0],
            recv_sem=sum_recv.at[0],
            device_id={"lon": peer},
            device_id_type=MESH,
        ).start()

    def send_edge(row, lon, lat):
        pltpu.make_async_remote_copy(
            src_ref=sums.at[row],
            dst_ref=cross.at[me],
            send_sem=send_sem.at[0],
            recv_sem=edge_recv.at[0],
            device_id={"lon": lon, "lat": lat},
            device_id_type=MESH,
        ).start()

    def to_hubs(act, *args):
        for h in range(HUB):
            pl.when(me != h)(functools.partial(act, h, *args))

    def to_others(act, *args):
        for peer in peers:
            pl.when(peer >= HUB)(functools.partial(act, peer, *args))

    def open_to(peer):
        pl.semaphore_signal(go, inc=1, device_id={"lon": peer}, device_id_type=MESH)

    @pl.when(far)
    def _():
        pl.semaphore_wait(barrier, lon_count - 1)
        for h in range(HUB):
            open_to(h)

    sums[0] = jnp.zeros((1, width), jnp.float32)
    sums[row_count + 1] = jnp.zeros((1, width), jnp.float32)
    get_bracket.wait()
    get_fraction.wait()
    whole = pl.ds(0, var_count)
    for pair in range(pair_count):
        pltpu.make_async_copy(fields.at[pair], fields.at[pair], field_sem.at[pair]).wait()
        some = pl.ds(2 * pair, 2)
        parts = PARTS[pair]
        for part in range(parts):
            count_here = plev_count // parts
            low = part * count_here
            interpolate(pair, range(low, low + count_here), fields, bracket, fraction, send)

            if pair == pair_count - 1 and part == parts - 1:
                continue

            @pl.when(early)
            def _():
                if pair == 0 and part == 0:
                    pl.when(late)(lambda: pl.semaphore_wait(barrier, HUB))
                send_block(0, some, pl.ds(low, count_here))
                if pair == 0 and part == parts - 1:
                    pl.when(jnp.logical_or(late, last))(functools.partial(send_block, 1, some))

    ones = jnp.ones((TILE, lons), jnp.bfloat16)

    def add_up(at):
        two = jnp.concatenate([send[:, at + r].reshape(width, lons) for r in range(2)])
        total = lax.dot_general(
            ones, two, (((1,), (1,)), ((), ())), preferred_element_type=jnp.float32
        )
        sums[at + 1] = total[0:1, :width]
        sums[at + 2] = total[0:1, width:]

    if row_count == TILE:
        for at in range(0, row_count, 2):
            add_up(at)
    else:
        pl.loop(0, row_count // 2)(lambda half: add_up(2 * half))

    def send_edges():
        pl.when(up)(lambda: send_edge(row_count, 0, next_band))
        pl.when(down)(lambda: send_edge(1, lon_count - 1, prev_band))

    beyond = up.astype(jnp.int32) + down.astype(jnp.int32)
    beside = jnp.logical_and(full, jnp.logical_not(hub))

    def choose(group, act, *args):
        for peer, aside in others:
            distant = peer >= lon_count - 2
            wanted = {
                "far": distant,
                "near": jnp.logical_not(jnp.logical_or(distant, peer < HUB)),
                "aside": jnp.logical_and(peer >= HUB, aside),
                "rest": jnp.logical_and(peer >= HUB, jnp.logical_not(aside)),
            }[group]
            pl.when(wanted)(functools.partial(act, peer, *args))

    def send_edges():
        pl.when(up)(lambda: send_edge(row_count, 0, next_band))
        pl.when(down)(lambda: send_edge(1, lon_count - 1, prev_band))

    @pl.when(hub)
    def _():
        pl.semaphore_wait(barrier, lon_count - 3 + beyond)
        choose("near", send_block, whole)
        to_hubs(send_sums)
        choose("near", send_sums)
        pl.when(me == 1)(functools.partial(send_block, 0, whole))
        pl.when(me == 0)(functools.partial(send_block, 1, whole))
        pl.semaphore_wait(go, 2)
        send_edges()
        choose("far", send_sums)
        choose("far", send_block, whole)

    @pl.when(beside)
    def _():
        pl.semaphore_wait(barrier, lon_count - 1 + beyond)
        open_to(me + 1)

        @pl.when(me == lon_count - 4)
        def _():
            open_to(lon_count - 2)
            open_to(lon_count - 1)

        to_hubs(send_sums)
        send_edges()
        to_others(send_sums)
        send_block(0, whole)
        choose("aside", send_block, whole)
        send_block(1, whole)
        choose("rest", send_block, whole)

    @pl.when(early)
    def _():
        send_sums(0)
        send_block(0, some, pl.ds(low, count_here))
        send_sums(1)
        for pair in range(1, pair_count):
            pl.when(late)(functools.partial(send_block, 1, pl.ds(2 * pair, 2)))

        @pl.when(far)
        def _():
            pl.when(last)(functools.partial(send_block, 1, pl.ds(2, var_count - 2)))
            pl.when(jnp.logical_not(last))(functools.partial(send_block, 1, whole))
            to_others(send_sums)
            to_others(send_block, whole)

        pl.semaphore_wait(go, 1)
        send_edges()

        @pl.when(late)
        def _():
            to_others(send_sums)
            to_others(send_block, whole)

    out_ref[:, :, :, my_lons] = send[:, pl.ds(me * own, own)]
    got[me] = sums[pl.ds(me * own, own + 2)]
    all_sums = got.at[pl.ds(0, lon_count - 1)]
    pltpu.make_async_copy(all_sums, all_sums, sum_recv.at[0]).wait()

    @pl.when(jnp.logical_or(jnp.logical_and(first, down), jnp.logical_and(last, up)))
    def _():
        pltpu.make_async_copy(cross, cross, edge_recv.at[0]).wait()

    def mean_of(parts):
        total = parts[0]
        for part in parts[1:]:
            total = total + part
        return total * (1 / count) if math.frexp(count)[0] == 0.5 else total / count

    here = [mean_of([got[l, j] for l in range(lon_count)]) for j in range(own + 2)]
    beyond_edge = mean_of([cross[l] for l in range(lon_count)])
    bottom = jnp.logical_and(first, band == 0)
    top = jnp.logical_and(last, band == lat_count - 1)
    for j in range(own):
        below, middle, above = here[j : j + 3]
        scale = jnp.float32(0.5)
        if j == 0:
            below = jnp.where(bottom, middle, jnp.where(first, beyond_edge, below))
            scale = jnp.where(bottom, 1.0, scale)
        if j == own - 1:
            above = jnp.where(top, middle, jnp.where(last, beyond_edge, above))
            scale = jnp.where(top, 1.0, scale)
        slope = scale * (above - below)
        for v in range(var_count):
            some = slice(v * plev_count, (v + 1) * plev_count)
            zonal[v, j : j + 1, :] = middle[:, some]
            merid[v, j : j + 1, :] = slope[:, some]

    pltpu.make_async_copy(all_sums, all_sums, send_sem.at[0]).wait()

    @pl.when(jnp.logical_and(up, down))
    def _():
        two = sums.at[pl.ds(0, 2)]
        pltpu.make_async_copy(two, two, send_sem.at[0]).wait()

    @pl.when(up != down)
    def _():
        one = sums.at[pl.ds(0, 1)]
        pltpu.make_async_copy(one, one, send_sem.at[0]).wait()

    landed = out_ref.at[:, :, :, pl.ds(0, (lon_count - 1) * lons)]
    pltpu.make_async_copy(landed, landed, recv_sem.at[0]).wait()
    left = send.at[:, pl.ds(0, row_count - own)]
    pltpu.make_async_copy(left, left, send_sem.at[0]).wait()


def finish(rows_vmem, zonal_vmem, merid_vmem, out_hbm, zonal_hbm, merid_hbm, sem):
    puts = [
        pltpu.make_async_copy(zonal_vmem, zonal_hbm, sem.at[1]),
        pltpu.make_async_copy(merid_vmem, merid_hbm, sem.at[2]),
    ]
    for put in puts:
        put.start()
    for v in range(rows_vmem.shape[0]):
        pltpu.make_async_copy(rows_vmem.at[v], out_hbm.at[v], sem.at[0]).start()
    for put in puts:
        put.wait()
    pltpu.make_async_copy(rows_vmem, out_hbm, sem.at[0]).wait()


def shards(lon_count, lat_count, fields, bracket, fraction):
    var_count, level_count, row_count, lons = fields.shape
    plev_count = bracket.shape[0]
    own = row_count // lon_count
    width = var_count * plev_count
    dma = pltpu.SemaphoreType.DMA
    anywhere = pl.BlockSpec(memory_space=pl.ANY)
    room = 2 * fields.size + 4 * bracket.size + 2 * fraction.size * (1 + var_count)
    in_vmem = pl.BlockSpec(memory_space=pltpu.VMEM)
    rows_shape = (var_count, own, plev_count, lons * lon_count)
    mean_shape = (var_count, own, plev_count)
    inputs = [pltpu.with_memory_space_constraint(x, pltpu.HBM) for x in (fields, bracket, fraction)]
    held = pl.pallas_call(
        functools.partial(exchange, lon_count, lat_count, float(lons * lon_count)),
        out_shape=(
            pltpu.VMEM(rows_shape, jnp.bfloat16),
            pltpu.VMEM(mean_shape, jnp.float32),
            pltpu.VMEM(mean_shape, jnp.float32),
        ),
        in_specs=[anywhere] * 3,
        out_specs=(in_vmem,) * 3,
        scratch_shapes=[
            pltpu.VMEM((var_count // 2, level_count, 2 * row_count, lons), fields.dtype),
            pltpu.VMEM(bracket.shape, bracket.dtype),
            pltpu.VMEM(fraction.shape, fraction.dtype),
            pltpu.VMEM((var_count, row_count, plev_count, lons), jnp.bfloat16),
            pltpu.VMEM((row_count + 2, 1, width), jnp.float32),
            pltpu.VMEM((lon_count, own + 2, 1, width), jnp.float32),
            pltpu.VMEM((lon_count, 1, width), jnp.float32),
            dma((1,)),
            dma((var_count // 2,)),
            dma((1,)),
            dma((1,)),
            dma((1,)),
            dma((1,)),
            pltpu.SemaphoreType.REGULAR,
        ],
        compiler_params=pltpu.CompilerParams(
            collective_id=0, has_side_effects=True, vmem_limit_bytes=room + (8 << 20)
        ),
    )(*inputs)
    held = [pltpu.with_memory_space_constraint(x, pltpu.VMEM) for x in held]
    on_pressure, zonal_mean, meridional = pl.pallas_call(
        finish,
        out_shape=(
            jax.ShapeDtypeStruct(rows_shape, jnp.bfloat16),
            jax.ShapeDtypeStruct(mean_shape, jnp.float32),
            jax.ShapeDtypeStruct(mean_shape, jnp.float32),
        ),
        in_specs=[in_vmem] * 3,
        out_specs=(anywhere,) * 3,
        scratch_shapes=[dma((3,))],
        compiler_params=pltpu.CompilerParams(vmem_limit_bytes=8 << 20),
    )(*held)
    return (
        on_pressure.transpose(0, 2, 1, 3),
        zonal_mean.transpose(0, 2, 1),
        meridional.transpose(0, 2, 1),
    )


def solution(mesh):
    return jax.shard_map(
        functools.partial(shards, mesh.shape["lon"], mesh.shape["lat"]),
        mesh=mesh,
        in_specs=(P(None, None, "lat", "lon"), P(None, "lat", "lon"), P(None, "lat", "lon")),
        out_specs=(
            P(None, None, ("lat", "lon"), None),
            P(None, None, ("lat", "lon")),
            P(None, None, ("lat", "lon")),
        ),
        check_vma=False,
    )
```

```python
import functools
import math

import jax
import jax.numpy as jnp
from jax import lax
from jax.experimental import pallas as pl
from jax.experimental.pallas import tpu as pltpu
from jax.sharding import PartitionSpec as P

WINDOW = 16
TILE = 8
PACK = 16
MESH = pl.DeviceIdType.MESH
HUB = 2
PARTS = (2, 2)


def select_pair(levels, masks):
    bit = len(levels) // 2
    for mask in masks:
        levels = [
            jnp.where(mask, levels[k + bit], levels[k]) if k + bit < len(levels) else levels[k]
            for k in range(bit + 1)
        ]
        bit //= 2
    return levels


def partner(me, k, count):
    if count & (count - 1):
        return (me + k) % count, (me + count - k) % count
    peer, bit = me, 1
    while bit < count:
        if k & bit:
            peer = peer + bit - 2 * bit * ((me // bit) % 2)
        bit *= 2
    return peer, peer


def interpolate(pair, levels, fields, bracket, fraction, send):
    _, level_count, both_rows, lons = fields.shape
    plev_count, row_count, _ = bracket.shape
    level_step = level_count // plev_count
    group_size = min(TILE, plev_count)

    def block(tile):
        where = [tile * PACK + half for half in range(0, PACK, TILE)]
        rows = [pl.ds(pl.multiple_of(at % row_count, TILE), TILE) for at in where]
        packed = pl.ds(pl.multiple_of(tile * PACK, PACK), PACK)
        loaded, groups = {}, [[], []]
        for p in levels:
            base = min(p * level_step, level_count - WINDOW)
            for k in range(base, base + WINDOW):
                if k not in loaded:
                    loaded[k] = fields[pair, k, packed, :]
            offset = (jnp.concatenate([bracket[p, r, :] for r in rows]) - base).astype(jnp.int16)
            masks, bit = [offset >= jnp.int16(WINDOW // 2)], WINDOW // 4
            while bit:
                masks.append((offset & jnp.int16(bit)) != jnp.int16(0))
                bit //= 2
            lower, upper = select_pair([loaded[base + k] for k in range(WINDOW)], masks)
            lower, upper = lower.astype(jnp.float32), upper.astype(jnp.float32)
            weight = jnp.concatenate([fraction[p, r, :].astype(jnp.float32) for r in rows])
            value = (lower + weight * (upper - lower)).astype(jnp.bfloat16)
            groups[0].append(value[:TILE])
            groups[1].append(value[TILE:])
            if len(groups[0]) == group_size:
                for half in range(2):
                    by_row = jnp.transpose(jnp.stack(groups[half]), (1, 0, 2))
                    v = 2 * pair + where[half] // row_count
                    send[v, rows[half], p + 1 - group_size : p + 1, :] = by_row
                groups = [[], []]

    if both_rows == PACK:
        block(0)
    else:
        pl.loop(0, both_rows // PACK)(block)


def exchange(
    lon_count, lat_count, count, fields_hbm, bracket_hbm, fraction_hbm,
    out_ref, zonal, merid,
    fields, bracket, fraction, send, sums, got, cross,
    in_sem, field_sem, send_sem, recv_sem, sum_recv, edge_recv, go,
):
    var_count, row_count, plev_count, lons = send.shape
    pair_count = var_count // 2
    own = row_count // lon_count
    width = var_count * plev_count
    me = lax.axis_index("lon")
    band = lax.axis_index("lat")
    next_band = (band + 1) % lat_count
    prev_band = (band + lat_count - 1) % lat_count
    first = me == 0
    last = me == lon_count - 1
    up = band < lat_count - 1
    down = band > 0
    my_lons = pl.ds(pl.multiple_of(me * lons, 128), lons)
    steps = range(lon_count - 1, 0, -1)
    peers = [partner(me, k, lon_count)[0] for k in steps]
    others = [(peer, (me // 2) % 2 != (k // 2) % 2) for k, peer in zip(steps, peers)]
    hub = me < HUB
    far = me >= lon_count - 2
    late = jnp.logical_and(me % 2 == 1, jnp.logical_not(jnp.logical_or(hub, far)))
    early = jnp.logical_or(far, late)
    full = jnp.logical_not(early)

    get_bracket = pltpu.make_async_copy(bracket_hbm, bracket, in_sem.at[0])
    get_fraction = pltpu.make_async_copy(fraction_hbm, fraction, in_sem.at[0])
    get_bracket.start()
    get_fraction.start()

    def get_pair(pair):
        for half in range(2):
            pltpu.make_async_copy(
                fields_hbm.at[2 * pair + half],
                fields.at[pair, :, pl.ds(half * row_count, row_count)],
                field_sem.at[pair],
            ).start()

    for pair in range(pair_count):
        get_pair(pair)

    barrier = pltpu.get_barrier_semaphore()

    def greet(peer, lat):
        pl.semaphore_signal(barrier, inc=1, device_id={"lon": peer, "lat": lat}, device_id_type=MESH)

    for peer in peers:
        listens = jnp.logical_or(jnp.logical_or(hub, peer % 2 == 0), jnp.logical_or(peer < HUB, peer >= lon_count - 2))
        apart = jnp.logical_and(far, peer < HUB)
        pl.when(jnp.logical_and(listens, jnp.logical_not(apart)))(functools.partial(greet, peer, band))

    waiting = [l for l in range(lon_count - 2) if l < HUB or l % 2 == 0]

    @pl.when(jnp.logical_and(first, down))
    def _():
        for l in waiting:
            greet(l, prev_band)

    @pl.when(jnp.logical_and(last, up))
    def _():
        for l in waiting:
            greet(l, next_band)

    def send_block(peer, some, levels=slice(None)):
        pltpu.make_async_remote_copy(
            src_ref=send.at[some, pl.ds(peer * own, own), levels],
            dst_ref=out_ref.at[some, :, levels, my_lons],
            send_sem=send_sem.at[0],
            recv_sem=recv_sem.at[0],
            device_id={"lon": peer},
            device_id_type=MESH,
        ).start()

    def send_sums(peer):
        pltpu.make_async_remote_copy(
            src_ref=sums.at[pl.ds(peer * own, own + 2)],
            dst_ref=got.at[me],
            send_sem=send_sem.at[0],
            recv_sem=sum_recv.at[0],
            device_id={"lon": peer},
            device_id_type=MESH,
        ).start()

    def send_edge(row, lon, lat):
        pltpu.make_async_remote_copy(
            src_ref=sums.at[row],
            dst_ref=cross.at[me],
            send_sem=send_sem.at[0],
            recv_sem=edge_recv.at[0],
            device_id={"lon": lon, "lat": lat},
            device_id_type=MESH,
        ).start()

    def to_hubs(act, *args):
        for h in range(HUB):
            pl.when(me != h)(functools.partial(act, h, *args))

    def to_others(act, *args):
        for peer in peers:
            pl.when(peer >= HUB)(functools.partial(act, peer, *args))

    def open_to(peer):
        pl.semaphore_signal(go, inc=1, device_id={"lon": peer}, device_id_type=MESH)

    @pl.when(far)
    def _():
        pl.semaphore_wait(barrier, lon_count - 1)
        for h in range(HUB):
            open_to(h)

    sums[0] = jnp.zeros((1, width), jnp.float32)
    sums[row_count + 1] = jnp.zeros((1, width), jnp.float32)
    get_bracket.wait()
    get_fraction.wait()
    whole = pl.ds(0, var_count)
    for pair in range(pair_count):
        pltpu.make_async_copy(fields.at[pair], fields.at[pair], field_sem.at[pair]).wait()
        some = pl.ds(2 * pair, 2)
        parts = PARTS[pair]
        for part in range(parts):
            count_here = plev_count // parts
            low = part * count_here
            interpolate(pair, range(low, low + count_here), fields, bracket, fraction, send)

            if pair == pair_count - 1 and part == parts - 1:
                continue

            @pl.when(early)
            def _():
                if pair == 0 and part == 0:
                    pl.when(late)(lambda: pl.semaphore_wait(barrier, HUB))
                send_block(0, some, pl.ds(low, count_here))
                if pair == 0 and part == parts - 1:
                    pl.when(jnp.logical_or(late, last))(functools.partial(send_block, 1, some))

    ones = jnp.ones((TILE, lons), jnp.bfloat16)

    def add_up(at):
        two = jnp.concatenate([send[:, at + r].reshape(width, lons) for r in range(2)])
        total = lax.dot_general(
            ones, two, (((1,), (1,)), ((), ())), preferred_element_type=jnp.float32
        )
        sums[at + 1] = total[0:1, :width]
        sums[at + 2] = total[0:1, width:]

    if row_count == TILE:
        for at in range(0, row_count, 2):
            add_up(at)
    else:
        pl.loop(0, row_count // 2)(lambda half: add_up(2 * half))

    def send_edges():
        pl.when(up)(lambda: send_edge(row_count, 0, next_band))
        pl.when(down)(lambda: send_edge(1, lon_count - 1, prev_band))

    beyond = up.astype(jnp.int32) + down.astype(jnp.int32)
    beside = jnp.logical_and(full, jnp.logical_not(hub))

    def choose(group, act, *args):
        for peer, aside in others:
            distant = peer >= lon_count - 2
            wanted = {
                "far": distant,
                "near": jnp.logical_not(jnp.logical_or(distant, peer < HUB)),
                "aside": jnp.logical_and(peer >= HUB, aside),
                "rest": jnp.logical_and(peer >= HUB, jnp.logical_not(aside)),
            }[group]
            pl.when(wanted)(functools.partial(act, peer, *args))

    def send_edges():
        pl.when(up)(lambda: send_edge(row_count, 0, next_band))
        pl.when(down)(lambda: send_edge(1, lon_count - 1, prev_band))

    @pl.when(hub)
    def _():
        pl.semaphore_wait(barrier, lon_count - 3 + beyond)
        choose("near", send_block, whole)
        to_hubs(send_sums)
        choose("near", send_sums)
        pl.when(me == 1)(functools.partial(send_block, 0, whole))
        pl.when(me == 0)(functools.partial(send_block, 1, whole))
        pl.semaphore_wait(go, 2)
        send_edges()
        choose("far", send_sums)
        choose("far", send_block, whole)

    @pl.when(beside)
    def _():
        pl.semaphore_wait(barrier, lon_count - 1 + beyond)
        open_to(me + 1)

        @pl.when(me == lon_count - 4)
        def _():
            open_to(lon_count - 2)
            open_to(lon_count - 1)

        to_hubs(send_sums)
        send_edges()
        to_others(send_sums)
        send_block(0, whole)
        choose("aside", send_block, whole)
        send_block(1, whole)
        choose("rest", send_block, whole)

    @pl.when(early)
    def _():
        send_sums(0)
        send_block(0, some, pl.ds(low, count_here))
        send_sums(1)
        for pair in range(1, pair_count):
            pl.when(late)(functools.partial(send_block, 1, pl.ds(2 * pair, 2)))

        @pl.when(far)
        def _():
            pl.when(last)(functools.partial(send_block, 1, pl.ds(2, var_count - 2)))
            pl.when(jnp.logical_not(last))(functools.partial(send_block, 1, whole))
            to_others(send_sums)
            to_others(send_block, whole)

        pl.semaphore_wait(go, 1)
        send_edges()

        @pl.when(late)
        def _():
            to_others(send_sums)
            to_others(send_block, whole)

    out_ref[:, :, :, my_lons] = send[:, pl.ds(me * own, own)]
    got[me] = sums[pl.ds(me * own, own + 2)]
    all_sums = got.at[pl.ds(0, lon_count - 1)]
    pltpu.make_async_copy(all_sums, all_sums, sum_recv.at[0]).wait()

    @pl.when(jnp.logical_or(jnp.logical_and(first, down), jnp.logical_and(last, up)))
    def _():
        pltpu.make_async_copy(cross, cross, edge_recv.at[0]).wait()

    def mean_of(parts):
        total = parts[0]
        for part in parts[1:]:
            total = total + part
        return total * (1 / count) if math.frexp(count)[0] == 0.5 else total / count

    here = [mean_of([got[l, j] for l in range(lon_count)]) for j in range(own + 2)]
    beyond_edge = mean_of([cross[l] for l in range(lon_count)])
    bottom = jnp.logical_and(first, band == 0)
    top = jnp.logical_and(last, band == lat_count - 1)
    for j in range(own):
        below, middle, above = here[j : j + 3]
        scale = jnp.float32(0.5)
        if j == 0:
            below = jnp.where(bottom, middle, jnp.where(first, beyond_edge, below))
            scale = jnp.where(bottom, 1.0, scale)
        if j == own - 1:
            above = jnp.where(top, middle, jnp.where(last, beyond_edge, above))
            scale = jnp.where(top, 1.0, scale)
        slope = scale * (above - below)
        for v in range(var_count):
            some = slice(v * plev_count, (v + 1) * plev_count)
            zonal[v, j : j + 1, :] = middle[:, some]
            merid[v, j : j + 1, :] = slope[:, some]

    pltpu.make_async_copy(all_sums, all_sums, send_sem.at[0]).wait()

    @pl.when(jnp.logical_and(up, down))
    def _():
        two = sums.at[pl.ds(0, 2)]
        pltpu.make_async_copy(two, two, send_sem.at[0]).wait()

    @pl.when(up != down)
    def _():
        one = sums.at[pl.ds(0, 1)]
        pltpu.make_async_copy(one, one, send_sem.at[0]).wait()

    landed = out_ref.at[:, :, :, pl.ds(0, (lon_count - 1) * lons)]
    pltpu.make_async_copy(landed, landed, recv_sem.at[0]).wait()
    left = send.at[:, pl.ds(0, row_count - own)]
    pltpu.make_async_copy(left, left, send_sem.at[0]).wait()


def finish(rows_vmem, zonal_vmem, merid_vmem, out_hbm, zonal_hbm, merid_hbm, sem):
    puts = [
        pltpu.make_async_copy(zonal_vmem, zonal_hbm, sem.at[0]),
        pltpu.make_async_copy(merid_vmem, merid_hbm, sem.at[0]),
    ]
    for put in puts:
        put.start()
    for v in range(rows_vmem.shape[0]):
        pltpu.make_async_copy(rows_vmem.at[v], out_hbm.at[v], sem.at[0]).start()
    for put in puts:
        put.wait()
    pltpu.make_async_copy(rows_vmem, out_hbm, sem.at[0]).wait()


def shards(lon_count, lat_count, fields, bracket, fraction):
    var_count, level_count, row_count, lons = fields.shape
    plev_count = bracket.shape[0]
    own = row_count // lon_count
    width = var_count * plev_count
    dma = pltpu.SemaphoreType.DMA
    anywhere = pl.BlockSpec(memory_space=pl.ANY)
    room = 2 * fields.size + 4 * bracket.size + 2 * fraction.size * (1 + var_count)
    in_vmem = pl.BlockSpec(memory_space=pltpu.VMEM)
    rows_shape = (var_count, own, plev_count, lons * lon_count)
    mean_shape = (var_count, own, plev_count)
    inputs = [pltpu.with_memory_space_constraint(x, pltpu.HBM) for x in (fields, bracket, fraction)]
    held = pl.pallas_call(
        functools.partial(exchange, lon_count, lat_count, float(lons * lon_count)),
        out_shape=(
            pltpu.VMEM(rows_shape, jnp.bfloat16),
            pltpu.VMEM(mean_shape, jnp.float32),
            pltpu.VMEM(mean_shape, jnp.float32),
        ),
        in_specs=[anywhere] * 3,
        out_specs=(in_vmem,) * 3,
        scratch_shapes=[
            pltpu.VMEM((var_count // 2, level_count, 2 * row_count, lons), fields.dtype),
            pltpu.VMEM(bracket.shape, bracket.dtype),
            pltpu.VMEM(fraction.shape, fraction.dtype),
            pltpu.VMEM((var_count, row_count, plev_count, lons), jnp.bfloat16),
            pltpu.VMEM((row_count + 2, 1, width), jnp.float32),
            pltpu.VMEM((lon_count, own + 2, 1, width), jnp.float32),
            pltpu.VMEM((lon_count, 1, width), jnp.float32),
            dma((1,)),
            dma((var_count // 2,)),
            dma((1,)),
            dma((1,)),
            dma((1,)),
            dma((1,)),
            pltpu.SemaphoreType.REGULAR,
        ],
        compiler_params=pltpu.CompilerParams(
            collective_id=0, has_side_effects=True, vmem_limit_bytes=room + (8 << 20)
        ),
    )(*inputs)
    held = [pltpu.with_memory_space_constraint(x, pltpu.VMEM) for x in held]
    on_pressure, zonal_mean, meridional = pl.pallas_call(
        finish,
        out_shape=(
            jax.ShapeDtypeStruct(rows_shape, jnp.bfloat16),
            jax.ShapeDtypeStruct(mean_shape, jnp.float32),
            jax.ShapeDtypeStruct(mean_shape, jnp.float32),
        ),
        in_specs=[in_vmem] * 3,
        out_specs=(anywhere,) * 3,
        scratch_shapes=[dma((1,))],
        compiler_params=pltpu.CompilerParams(vmem_limit_bytes=8 << 20),
    )(*held)
    return (
        on_pressure.transpose(0, 2, 1, 3),
        zonal_mean.transpose(0, 2, 1),
        meridional.transpose(0, 2, 1),
    )


def solution(mesh):
    return jax.shard_map(
        functools.partial(shards, mesh.shape["lon"], mesh.shape["lat"]),
        mesh=mesh,
        in_specs=(P(None, None, "lat", "lon"), P(None, "lat", "lon"), P(None, "lat", "lon")),
        out_specs=(
            P(None, None, ("lat", "lon"), None),
            P(None, None, ("lat", "lon")),
            P(None, None, ("lat", "lon")),
        ),
        check_vma=False,
    )
```

```python
import functools
import math

import jax
import jax.numpy as jnp
from jax import lax
from jax.experimental import pallas as pl
from jax.experimental.pallas import tpu as pltpu
from jax.sharding import PartitionSpec as P

WINDOW = 16
TILE = 8
PACK = 16
MESH = pl.DeviceIdType.MESH
HUB = 2
PARTS = (2, 4)


def select_pair(levels, masks):
    bit = len(levels) // 2
    for mask in masks:
        levels = [
            jnp.where(mask, levels[k + bit], levels[k]) if k + bit < len(levels) else levels[k]
            for k in range(bit + 1)
        ]
        bit //= 2
    return levels


def partner(me, k, count):
    if count & (count - 1):
        return (me + k) % count, (me + count - k) % count
    peer, bit = me, 1
    while bit < count:
        if k & bit:
            peer = peer + bit - 2 * bit * ((me // bit) % 2)
        bit *= 2
    return peer, peer


def interpolate(pair, levels, fields, bracket, fraction, send):
    _, level_count, both_rows, lons = fields.shape
    plev_count, row_count, _ = bracket.shape
    level_step = level_count // plev_count
    group_size = min(TILE, plev_count)

    def block(tile):
        where = [tile * PACK + half for half in range(0, PACK, TILE)]
        rows = [pl.ds(pl.multiple_of(at % row_count, TILE), TILE) for at in where]
        packed = pl.ds(pl.multiple_of(tile * PACK, PACK), PACK)
        loaded, groups = {}, [[], []]
        for p in levels:
            base = min(p * level_step, level_count - WINDOW)
            for k in range(base, base + WINDOW):
                if k not in loaded:
                    loaded[k] = fields[pair, k, packed, :]
            offset = (jnp.concatenate([bracket[p, r, :] for r in rows]) - base).astype(jnp.int16)
            masks, bit = [offset >= jnp.int16(WINDOW // 2)], WINDOW // 4
            while bit:
                masks.append((offset & jnp.int16(bit)) != jnp.int16(0))
                bit //= 2
            lower, upper = select_pair([loaded[base + k] for k in range(WINDOW)], masks)
            lower, upper = lower.astype(jnp.float32), upper.astype(jnp.float32)
            weight = jnp.concatenate([fraction[p, r, :].astype(jnp.float32) for r in rows])
            value = (lower + weight * (upper - lower)).astype(jnp.bfloat16)
            groups[0].append(value[:TILE])
            groups[1].append(value[TILE:])
            if len(groups[0]) == group_size:
                for half in range(2):
                    by_row = jnp.transpose(jnp.stack(groups[half]), (1, 0, 2))
                    v = 2 * pair + where[half] // row_count
                    send[v, rows[half], p + 1 - group_size : p + 1, :] = by_row
                groups = [[], []]

    if both_rows == PACK:
        block(0)
    else:
        pl.loop(0, both_rows // PACK)(block)


def exchange(
    lon_count, lat_count, count, fields_hbm, bracket_hbm, fraction_hbm,
    out_ref, zonal, merid,
    fields, bracket, fraction, send, sums, got, cross,
    in_sem, field_sem, send_sem, recv_sem, sum_recv, edge_recv, go,
):
    var_count, row_count, plev_count, lons = send.shape
    pair_count = var_count // 2
    own = row_count // lon_count
    width = var_count * plev_count
    me = lax.axis_index("lon")
    band = lax.axis_index("lat")
    next_band = (band + 1) % lat_count
    prev_band = (band + lat_count - 1) % lat_count
    first = me == 0
    last = me == lon_count - 1
    up = band < lat_count - 1
    down = band > 0
    my_lons = pl.ds(pl.multiple_of(me * lons, 128), lons)
    steps = range(lon_count - 1, 0, -1)
    peers = [partner(me, k, lon_count)[0] for k in steps]
    others = [(peer, (me // 2) % 2 != (k // 2) % 2) for k, peer in zip(steps, peers)]
    hub = me < HUB
    far = me >= lon_count - 2
    late = jnp.logical_and(me % 2 == 1, jnp.logical_not(jnp.logical_or(hub, far)))
    early = jnp.logical_or(far, late)
    full = jnp.logical_not(early)

    get_bracket = pltpu.make_async_copy(bracket_hbm, bracket, in_sem.at[0])
    get_fraction = pltpu.make_async_copy(fraction_hbm, fraction, in_sem.at[0])
    get_bracket.start()
    get_fraction.start()

    def get_pair(pair):
        for half in range(2):
            pltpu.make_async_copy(
                fields_hbm.at[2 * pair + half],
                fields.at[pair, :, pl.ds(half * row_count, row_count)],
                field_sem.at[pair],
            ).start()

    for pair in range(pair_count):
        get_pair(pair)

    barrier = pltpu.get_barrier_semaphore()

    def greet(peer, lat):
        pl.semaphore_signal(barrier, inc=1, device_id={"lon": peer, "lat": lat}, device_id_type=MESH)

    for peer in peers:
        listens = jnp.logical_or(jnp.logical_or(hub, peer % 2 == 0), jnp.logical_or(peer < HUB, peer >= lon_count - 2))
        apart = jnp.logical_and(far, peer < HUB)
        pl.when(jnp.logical_and(listens, jnp.logical_not(apart)))(functools.partial(greet, peer, band))

    waiting = [l for l in range(lon_count - 2) if l < HUB or l % 2 == 0]

    @pl.when(jnp.logical_and(first, down))
    def _():
        for l in waiting:
            greet(l, prev_band)

    @pl.when(jnp.logical_and(last, up))
    def _():
        for l in waiting:
            greet(l, next_band)

    def send_block(peer, some, levels=slice(None)):
        pltpu.make_async_remote_copy(
            src_ref=send.at[some, pl.ds(peer * own, own), levels],
            dst_ref=out_ref.at[some, :, levels, my_lons],
            send_sem=send_sem.at[0],
            recv_sem=recv_sem.at[0],
            device_id={"lon": peer},
            device_id_type=MESH,
        ).start()

    def send_sums(peer):
        pltpu.make_async_remote_copy(
            src_ref=sums.at[pl.ds(peer * own, own + 2)],
            dst_ref=got.at[me],
            send_sem=send_sem.at[0],
            recv_sem=sum_recv.at[0],
            device_id={"lon": peer},
            device_id_type=MESH,
        ).start()

    def send_edge(row, lon, lat):
        pltpu.make_async_remote_copy(
            src_ref=sums.at[row],
            dst_ref=cross.at[me],
            send_sem=send_sem.at[0],
            recv_sem=edge_recv.at[0],
            device_id={"lon": lon, "lat": lat},
            device_id_type=MESH,
        ).start()

    def to_hubs(act, *args):
        for h in range(HUB):
            pl.when(me != h)(functools.partial(act, h, *args))

    def to_others(act, *args):
        for peer in peers:
            pl.when(peer >= HUB)(functools.partial(act, peer, *args))

    def open_to(peer):
        pl.semaphore_signal(go, inc=1, device_id={"lon": peer}, device_id_type=MESH)

    @pl.when(far)
    def _():
        pl.semaphore_wait(barrier, lon_count - 1)
        for h in range(HUB):
            open_to(h)

    sums[0] = jnp.zeros((1, width), jnp.float32)
    sums[row_count + 1] = jnp.zeros((1, width), jnp.float32)
    get_bracket.wait()
    get_fraction.wait()
    whole = pl.ds(0, var_count)
    for pair in range(pair_count):
        pltpu.make_async_copy(fields.at[pair], fields.at[pair], field_sem.at[pair]).wait()
        some = pl.ds(2 * pair, 2)
        parts = PARTS[pair]
        for part in range(parts):
            count_here = plev_count // parts
            low = part * count_here
            interpolate(pair, range(low, low + count_here), fields, bracket, fraction, send)

            if pair == pair_count - 1 and part == parts - 1:
                continue

            @pl.when(early)
            def _():
                if pair == 0 and part == 0:
                    pl.when(late)(lambda: pl.semaphore_wait(barrier, HUB))
                send_block(0, some, pl.ds(low, count_here))
                if pair == 0 and part == parts - 1:
                    pl.when(jnp.logical_or(late, last))(functools.partial(send_block, 1, some))

    ones = jnp.ones((TILE, lons), jnp.bfloat16)

    def add_up(at):
        two = jnp.concatenate([send[:, at + r].reshape(width, lons) for r in range(2)])
        total = lax.dot_general(
            ones, two, (((1,), (1,)), ((), ())), preferred_element_type=jnp.float32
        )
        sums[at + 1] = total[0:1, :width]
        sums[at + 2] = total[0:1, width:]

    if row_count == TILE:
        for at in range(0, row_count, 2):
            add_up(at)
    else:
        pl.loop(0, row_count // 2)(lambda half: add_up(2 * half))

    def send_edges():
        pl.when(up)(lambda: send_edge(row_count, 0, next_band))
        pl.when(down)(lambda: send_edge(1, lon_count - 1, prev_band))

    beyond = up.astype(jnp.int32) + down.astype(jnp.int32)
    beside = jnp.logical_and(full, jnp.logical_not(hub))

    def choose(group, act, *args):
        for peer, aside in others:
            distant = peer >= lon_count - 2
            wanted = {
                "far": distant,
                "near": jnp.logical_not(jnp.logical_or(distant, peer < HUB)),
                "aside": jnp.logical_and(peer >= HUB, aside),
                "rest": jnp.logical_and(peer >= HUB, jnp.logical_not(aside)),
            }[group]
            pl.when(wanted)(functools.partial(act, peer, *args))

    def send_edges():
        pl.when(up)(lambda: send_edge(row_count, 0, next_band))
        pl.when(down)(lambda: send_edge(1, lon_count - 1, prev_band))

    @pl.when(hub)
    def _():
        pl.semaphore_wait(barrier, lon_count - 3 + beyond)
        choose("near", send_block, whole)
        to_hubs(send_sums)
        choose("near", send_sums)
        pl.when(me == 1)(functools.partial(send_block, 0, whole))
        pl.when(me == 0)(functools.partial(send_block, 1, whole))
        pl.semaphore_wait(go, 2)
        send_edges()
        choose("far", send_sums)
        choose("far", send_block, whole)

    @pl.when(beside)
    def _():
        pl.semaphore_wait(barrier, lon_count - 1 + beyond)
        open_to(me + 1)

        @pl.when(me == lon_count - 4)
        def _():
            open_to(lon_count - 2)
            open_to(lon_count - 1)

        to_hubs(send_sums)
        send_block(0, whole)
        send_edges()
        to_others(send_sums)
        choose("aside", send_block, whole)
        send_block(1, whole)
        choose("rest", send_block, whole)

    @pl.when(early)
    def _():
        send_sums(0)
        send_block(0, some, pl.ds(low, count_here))
        send_sums(1)
        for pair in range(1, pair_count):
            pl.when(late)(functools.partial(send_block, 1, pl.ds(2 * pair, 2)))

        @pl.when(far)
        def _():
            pl.when(last)(functools.partial(send_block, 1, pl.ds(2, var_count - 2)))
            pl.when(jnp.logical_not(last))(functools.partial(send_block, 1, whole))
            to_others(send_sums)
            to_others(send_block, whole)

        pl.semaphore_wait(go, 1)
        send_edges()

        @pl.when(late)
        def _():
            to_others(send_sums)
            to_others(send_block, whole)

    out_ref[:, :, :, my_lons] = send[:, pl.ds(me * own, own)]
    got[me] = sums[pl.ds(me * own, own + 2)]
    all_sums = got.at[pl.ds(0, lon_count - 1)]
    pltpu.make_async_copy(all_sums, all_sums, sum_recv.at[0]).wait()

    @pl.when(jnp.logical_or(jnp.logical_and(first, down), jnp.logical_and(last, up)))
    def _():
        pltpu.make_async_copy(cross, cross, edge_recv.at[0]).wait()

    def mean_of(parts):
        total = parts[0]
        for part in parts[1:]:
            total = total + part
        return total * (1 / count) if math.frexp(count)[0] == 0.5 else total / count

    here = [mean_of([got[l, j] for l in range(lon_count)]) for j in range(own + 2)]
    beyond_edge = mean_of([cross[l] for l in range(lon_count)])
    bottom = jnp.logical_and(first, band == 0)
    top = jnp.logical_and(last, band == lat_count - 1)
    for j in range(own):
        below, middle, above = here[j : j + 3]
        scale = jnp.float32(0.5)
        if j == 0:
            below = jnp.where(bottom, middle, jnp.where(first, beyond_edge, below))
            scale = jnp.where(bottom, 1.0, scale)
        if j == own - 1:
            above = jnp.where(top, middle, jnp.where(last, beyond_edge, above))
            scale = jnp.where(top, 1.0, scale)
        slope = scale * (above - below)
        for v in range(var_count):
            some = slice(v * plev_count, (v + 1) * plev_count)
            zonal[v, j : j + 1, :] = middle[:, some]
            merid[v, j : j + 1, :] = slope[:, some]

    pltpu.make_async_copy(all_sums, all_sums, send_sem.at[0]).wait()

    @pl.when(jnp.logical_and(up, down))
    def _():
        two = sums.at[pl.ds(0, 2)]
        pltpu.make_async_copy(two, two, send_sem.at[0]).wait()

    @pl.when(up != down)
    def _():
        one = sums.at[pl.ds(0, 1)]
        pltpu.make_async_copy(one, one, send_sem.at[0]).wait()

    landed = out_ref.at[:, :, :, pl.ds(0, (lon_count - 1) * lons)]
    pltpu.make_async_copy(landed, landed, recv_sem.at[0]).wait()
    left = send.at[:, pl.ds(0, row_count - own)]
    pltpu.make_async_copy(left, left, send_sem.at[0]).wait()


def finish(rows_vmem, zonal_vmem, merid_vmem, out_hbm, zonal_hbm, merid_hbm, sem):
    puts = [
        pltpu.make_async_copy(zonal_vmem, zonal_hbm, sem.at[0]),
        pltpu.make_async_copy(merid_vmem, merid_hbm, sem.at[0]),
    ]
    for put in puts:
        put.start()
    for v in range(rows_vmem.shape[0]):
        pltpu.make_async_copy(rows_vmem.at[v], out_hbm.at[v], sem.at[0]).start()
    for put in puts:
        put.wait()
    pltpu.make_async_copy(rows_vmem, out_hbm, sem.at[0]).wait()


def shards(lon_count, lat_count, fields, bracket, fraction):
    var_count, level_count, row_count, lons = fields.shape
    plev_count = bracket.shape[0]
    own = row_count // lon_count
    width = var_count * plev_count
    dma = pltpu.SemaphoreType.DMA
    anywhere = pl.BlockSpec(memory_space=pl.ANY)
    room = 2 * fields.size + 4 * bracket.size + 2 * fraction.size * (1 + var_count)
    in_vmem = pl.BlockSpec(memory_space=pltpu.VMEM)
    rows_shape = (var_count, own, plev_count, lons * lon_count)
    mean_shape = (var_count, own, plev_count)
    inputs = [pltpu.with_memory_space_constraint(x, pltpu.HBM) for x in (fields, bracket, fraction)]
    held = pl.pallas_call(
        functools.partial(exchange, lon_count, lat_count, float(lons * lon_count)),
        out_shape=(
            pltpu.VMEM(rows_shape, jnp.bfloat16),
            pltpu.VMEM(mean_shape, jnp.float32),
            pltpu.VMEM(mean_shape, jnp.float32),
        ),
        in_specs=[anywhere] * 3,
        out_specs=(in_vmem,) * 3,
        scratch_shapes=[
            pltpu.VMEM((var_count // 2, level_count, 2 * row_count, lons), fields.dtype),
            pltpu.VMEM(bracket.shape, bracket.dtype),
            pltpu.VMEM(fraction.shape, fraction.dtype),
            pltpu.VMEM((var_count, row_count, plev_count, lons), jnp.bfloat16),
            pltpu.VMEM((row_count + 2, 1, width), jnp.float32),
            pltpu.VMEM((lon_count, own + 2, 1, width), jnp.float32),
            pltpu.VMEM((lon_count, 1, width), jnp.float32),
            dma((1,)),
            dma((var_count // 2,)),
            dma((1,)),
            dma((1,)),
            dma((1,)),
            dma((1,)),
            pltpu.SemaphoreType.REGULAR,
        ],
        compiler_params=pltpu.CompilerParams(
            collective_id=0, has_side_effects=True, vmem_limit_bytes=room + (8 << 20)
        ),
    )(*inputs)
    held = [pltpu.with_memory_space_constraint(x, pltpu.VMEM) for x in held]
    on_pressure, zonal_mean, meridional = pl.pallas_call(
        finish,
        out_shape=(
            jax.ShapeDtypeStruct(rows_shape, jnp.bfloat16),
            jax.ShapeDtypeStruct(mean_shape, jnp.float32),
            jax.ShapeDtypeStruct(mean_shape, jnp.float32),
        ),
        in_specs=[in_vmem] * 3,
        out_specs=(anywhere,) * 3,
        scratch_shapes=[dma((1,))],
        compiler_params=pltpu.CompilerParams(vmem_limit_bytes=8 << 20),
    )(*held)
    return (
        on_pressure.transpose(0, 2, 1, 3),
        zonal_mean.transpose(0, 2, 1),
        meridional.transpose(0, 2, 1),
    )


def solution(mesh):
    return jax.shard_map(
        functools.partial(shards, mesh.shape["lon"], mesh.shape["lat"]),
        mesh=mesh,
        in_specs=(P(None, None, "lat", "lon"), P(None, "lat", "lon"), P(None, "lat", "lon")),
        out_specs=(
            P(None, None, ("lat", "lon"), None),
            P(None, None, ("lat", "lon")),
            P(None, None, ("lat", "lon")),
        ),
        check_vma=False,
    )
```

```python
import functools
import math

import jax
import jax.numpy as jnp
from jax import lax
from jax.experimental import pallas as pl
from jax.experimental.pallas import tpu as pltpu
from jax.sharding import PartitionSpec as P

WINDOW = 16
TILE = 8
PACK = 16
MESH = pl.DeviceIdType.MESH
HUB = 2
PARTS = (2, 4)


def select_pair(levels, masks):
    bit = len(levels) // 2
    for mask in masks:
        levels = [
            jnp.where(mask, levels[k + bit], levels[k]) if k + bit < len(levels) else levels[k]
            for k in range(bit + 1)
        ]
        bit //= 2
    return levels


def partner(me, k, count):
    if count & (count - 1):
        return (me + k) % count, (me + count - k) % count
    peer, bit = me, 1
    while bit < count:
        if k & bit:
            peer = peer + bit - 2 * bit * ((me // bit) % 2)
        bit *= 2
    return peer, peer


def interpolate(pair, levels, fields, bracket, fraction, send):
    _, level_count, both_rows, lons = fields.shape
    plev_count, row_count, _ = bracket.shape
    level_step = level_count // plev_count
    group_size = min(TILE, plev_count)

    def block(tile):
        where = [tile * PACK + half for half in range(0, PACK, TILE)]
        rows = [pl.ds(pl.multiple_of(at % row_count, TILE), TILE) for at in where]
        packed = pl.ds(pl.multiple_of(tile * PACK, PACK), PACK)
        loaded, groups = {}, [[], []]
        for p in levels:
            base = min(p * level_step, level_count - WINDOW)
            for k in range(base, base + WINDOW):
                if k not in loaded:
                    loaded[k] = fields[pair, k, packed, :]
            offset = (jnp.concatenate([bracket[p, r, :] for r in rows]) - base).astype(jnp.int16)
            masks, bit = [offset >= jnp.int16(WINDOW // 2)], WINDOW // 4
            while bit:
                masks.append((offset & jnp.int16(bit)) != jnp.int16(0))
                bit //= 2
            lower, upper = select_pair([loaded[base + k] for k in range(WINDOW)], masks)
            lower, upper = lower.astype(jnp.float32), upper.astype(jnp.float32)
            weight = jnp.concatenate([fraction[p, r, :].astype(jnp.float32) for r in rows])
            value = (lower + weight * (upper - lower)).astype(jnp.bfloat16)
            groups[0].append(value[:TILE])
            groups[1].append(value[TILE:])
            if len(groups[0]) == group_size:
                for half in range(2):
                    by_row = jnp.transpose(jnp.stack(groups[half]), (1, 0, 2))
                    v = 2 * pair + where[half] // row_count
                    send[v, rows[half], p + 1 - group_size : p + 1, :] = by_row
                groups = [[], []]

    if both_rows == PACK:
        block(0)
    else:
        pl.loop(0, both_rows // PACK)(block)


def exchange(
    lon_count, lat_count, count, fields_hbm, bracket_hbm, fraction_hbm,
    out_ref, zonal, merid,
    fields, bracket, fraction, send, sums, got, cross,
    in_sem, field_sem, send_sem, recv_sem, sum_recv, edge_recv, go,
):
    var_count, row_count, plev_count, lons = send.shape
    pair_count = var_count // 2
    own = row_count // lon_count
    width = var_count * plev_count
    me = lax.axis_index("lon")
    band = lax.axis_index("lat")
    next_band = (band + 1) % lat_count
    prev_band = (band + lat_count - 1) % lat_count
    first = me == 0
    last = me == lon_count - 1
    up = band < lat_count - 1
    down = band > 0
    my_lons = pl.ds(pl.multiple_of(me * lons, 128), lons)
    steps = range(lon_count - 1, 0, -1)
    peers = [partner(me, k, lon_count)[0] for k in steps]
    others = [(peer, (me // 2) % 2 != (k // 2) % 2) for k, peer in zip(steps, peers)]
    hub = me < HUB
    far = me >= lon_count - 2
    late = jnp.logical_and(me % 2 == 1, jnp.logical_not(jnp.logical_or(hub, far)))
    early = jnp.logical_or(far, late)
    full = jnp.logical_not(early)

    get_bracket = pltpu.make_async_copy(bracket_hbm, bracket, in_sem.at[0])
    get_fraction = pltpu.make_async_copy(fraction_hbm, fraction, in_sem.at[0])
    get_bracket.start()
    get_fraction.start()

    def get_pair(pair):
        for half in range(2):
            pltpu.make_async_copy(
                fields_hbm.at[2 * pair + half],
                fields.at[pair, :, pl.ds(half * row_count, row_count)],
                field_sem.at[pair],
            ).start()

    for pair in range(pair_count):
        get_pair(pair)

    barrier = pltpu.get_barrier_semaphore()

    def greet(peer, lat):
        pl.semaphore_signal(barrier, inc=1, device_id={"lon": peer, "lat": lat}, device_id_type=MESH)

    for peer in peers:
        listens = jnp.logical_or(jnp.logical_or(hub, peer % 2 == 0), jnp.logical_or(peer < HUB, peer >= lon_count - 2))
        apart = jnp.logical_and(far, peer < HUB)
        pl.when(jnp.logical_and(listens, jnp.logical_not(apart)))(functools.partial(greet, peer, band))

    waiting = [l for l in range(lon_count - 2) if l < HUB or l % 2 == 0]

    @pl.when(jnp.logical_and(first, down))
    def _():
        for l in waiting:
            greet(l, prev_band)

    @pl.when(jnp.logical_and(last, up))
    def _():
        for l in waiting:
            greet(l, next_band)

    def send_block(peer, some, levels=slice(None)):
        pltpu.make_async_remote_copy(
            src_ref=send.at[some, pl.ds(peer * own, own), levels],
            dst_ref=out_ref.at[some, :, levels, my_lons],
            send_sem=send_sem.at[0],
            recv_sem=recv_sem.at[0],
            device_id={"lon": peer},
            device_id_type=MESH,
        ).start()

    def send_sums(peer):
        pltpu.make_async_remote_copy(
            src_ref=sums.at[pl.ds(peer * own, own + 2)],
            dst_ref=got.at[me],
            send_sem=send_sem.at[0],
            recv_sem=sum_recv.at[0],
            device_id={"lon": peer},
            device_id_type=MESH,
        ).start()

    def send_edge(row, lon, lat):
        pltpu.make_async_remote_copy(
            src_ref=sums.at[row],
            dst_ref=cross.at[me],
            send_sem=send_sem.at[0],
            recv_sem=edge_recv.at[0],
            device_id={"lon": lon, "lat": lat},
            device_id_type=MESH,
        ).start()

    def to_hubs(act, *args):
        for h in range(HUB):
            pl.when(me != h)(functools.partial(act, h, *args))

    def to_others(act, *args):
        for peer in peers:
            pl.when(peer >= HUB)(functools.partial(act, peer, *args))

    def open_to(peer):
        pl.semaphore_signal(go, inc=1, device_id={"lon": peer}, device_id_type=MESH)

    @pl.when(far)
    def _():
        pl.semaphore_wait(barrier, lon_count - 1)
        for h in range(HUB):
            open_to(h)

    sums[0] = jnp.zeros((1, width), jnp.float32)
    sums[row_count + 1] = jnp.zeros((1, width), jnp.float32)
    get_bracket.wait()
    get_fraction.wait()
    whole = pl.ds(0, var_count)
    for pair in range(pair_count):
        pltpu.make_async_copy(fields.at[pair], fields.at[pair], field_sem.at[pair]).wait()
        some = pl.ds(2 * pair, 2)
        parts = PARTS[pair]
        for part in range(parts):
            count_here = plev_count // parts
            low = part * count_here
            interpolate(pair, range(low, low + count_here), fields, bracket, fraction, send)

            if pair == pair_count - 1 and part == parts - 1:
                continue

            @pl.when(early)
            def _():
                if pair == 0 and part == 0:
                    pl.when(late)(lambda: pl.semaphore_wait(barrier, HUB))
                send_block(0, some, pl.ds(low, count_here))
                if pair == 0 and part == parts - 1:
                    pl.when(jnp.logical_or(late, last))(functools.partial(send_block, 1, some))

    ones = jnp.ones((TILE, lons), jnp.bfloat16)

    def add_up(at):
        two = jnp.concatenate([send[:, at + r].reshape(width, lons) for r in range(2)])
        total = lax.dot_general(
            ones, two, (((1,), (1,)), ((), ())), preferred_element_type=jnp.float32
        )
        sums[at + 1] = total[0:1, :width]
        sums[at + 2] = total[0:1, width:]

    if row_count == TILE:
        for at in range(0, row_count, 2):
            add_up(at)
    else:
        pl.loop(0, row_count // 2)(lambda half: add_up(2 * half))

    def send_edges():
        pl.when(up)(lambda: send_edge(row_count, 0, next_band))
        pl.when(down)(lambda: send_edge(1, lon_count - 1, prev_band))

    beyond = up.astype(jnp.int32) + down.astype(jnp.int32)
    beside = jnp.logical_and(full, jnp.logical_not(hub))

    def choose(group, act, *args):
        for peer, aside in others:
            distant = peer >= lon_count - 2
            wanted = {
                "far": distant,
                "near": jnp.logical_not(jnp.logical_or(distant, peer < HUB)),
                "aside": jnp.logical_and(peer >= HUB, aside),
                "rest": jnp.logical_and(peer >= HUB, jnp.logical_not(aside)),
            }[group]
            pl.when(wanted)(functools.partial(act, peer, *args))

    def send_edges():
        pl.when(up)(lambda: send_edge(row_count, 0, next_band))
        pl.when(down)(lambda: send_edge(1, lon_count - 1, prev_band))

    @pl.when(hub)
    def _():
        pl.semaphore_wait(barrier, lon_count - 3 + beyond)
        choose("near", send_block, whole)
        to_hubs(send_sums)
        choose("near", send_sums)
        pl.when(me == 1)(functools.partial(send_block, 0, whole))
        pl.when(me == 0)(functools.partial(send_block, 1, whole))
        pl.semaphore_wait(go, 2)
        send_edges()
        choose("far", send_sums)
        choose("far", send_block, whole)

    @pl.when(beside)
    def _():
        pl.semaphore_wait(barrier, lon_count - 1 + beyond)
        open_to(me + 1)

        @pl.when(me == lon_count - 4)
        def _():
            open_to(lon_count - 2)
            open_to(lon_count - 1)

        to_hubs(send_sums)
        send_edges()
        to_others(send_sums)
        send_block(0, whole)
        choose("aside", send_block, whole)
        send_block(1, whole)
        choose("rest", send_block, whole)

    @pl.when(early)
    def _():
        send_sums(0)
        send_block(0, some, pl.ds(low, count_here))
        send_sums(1)
        for pair in range(1, pair_count):
            pl.when(late)(functools.partial(send_block, 1, pl.ds(2 * pair, 2)))

        @pl.when(far)
        def _():
            pl.when(last)(functools.partial(send_block, 1, pl.ds(2, var_count - 2)))
            pl.when(jnp.logical_not(last))(functools.partial(send_block, 1, whole))
            to_others(send_sums)
            to_others(send_block, whole)

        pl.semaphore_wait(go, 1)
        send_edges()

        @pl.when(late)
        def _():
            to_others(send_sums)
            to_others(send_block, whole)

    out_ref[:, :, :, my_lons] = send[:, pl.ds(me * own, own)]
    got[me] = sums[pl.ds(me * own, own + 2)]
    all_sums = got.at[pl.ds(0, lon_count - 1)]
    pltpu.make_async_copy(all_sums, all_sums, sum_recv.at[0]).wait()

    @pl.when(jnp.logical_or(jnp.logical_and(first, down), jnp.logical_and(last, up)))
    def _():
        pltpu.make_async_copy(cross, cross, edge_recv.at[0]).wait()

    def mean_of(parts):
        total = parts[0]
        for part in parts[1:]:
            total = total + part
        return total * (1 / count) if math.frexp(count)[0] == 0.5 else total / count

    here = [mean_of([got[l, j] for l in range(lon_count)]) for j in range(own + 2)]
    beyond_edge = mean_of([cross[l] for l in range(lon_count)])
    bottom = jnp.logical_and(first, band == 0)
    top = jnp.logical_and(last, band == lat_count - 1)
    for j in range(own):
        below, middle, above = here[j : j + 3]
        scale = jnp.float32(0.5)
        if j == 0:
            below = jnp.where(bottom, middle, jnp.where(first, beyond_edge, below))
            scale = jnp.where(bottom, 1.0, scale)
        if j == own - 1:
            above = jnp.where(top, middle, jnp.where(last, beyond_edge, above))
            scale = jnp.where(top, 1.0, scale)
        slope = scale * (above - below)
        for v in range(var_count):
            some = slice(v * plev_count, (v + 1) * plev_count)
            zonal[v, j : j + 1, :] = middle[:, some]
            merid[v, j : j + 1, :] = slope[:, some]

    pltpu.make_async_copy(all_sums, all_sums, send_sem.at[0]).wait()

    @pl.when(jnp.logical_and(up, down))
    def _():
        two = sums.at[pl.ds(0, 2)]
        pltpu.make_async_copy(two, two, send_sem.at[0]).wait()

    @pl.when(up != down)
    def _():
        one = sums.at[pl.ds(0, 1)]
        pltpu.make_async_copy(one, one, send_sem.at[0]).wait()

    landed = out_ref.at[:, :, :, pl.ds(0, (lon_count - 1) * lons)]
    pltpu.make_async_copy(landed, landed, recv_sem.at[0]).wait()
    left = send.at[:, pl.ds(0, row_count - own)]
    pltpu.make_async_copy(left, left, send_sem.at[0]).wait()


def finish(rows_vmem, zonal_vmem, merid_vmem, out_hbm, zonal_hbm, merid_hbm, sem):
    puts = [
        pltpu.make_async_copy(zonal_vmem, zonal_hbm, sem.at[0]),
        pltpu.make_async_copy(merid_vmem, merid_hbm, sem.at[0]),
    ]
    for put in puts:
        put.start()
    for v in range(rows_vmem.shape[0]):
        pltpu.make_async_copy(rows_vmem.at[v], out_hbm.at[v], sem.at[0]).start()
    for put in puts:
        put.wait()
    pltpu.make_async_copy(rows_vmem, out_hbm, sem.at[0]).wait()


def shards(lon_count, lat_count, fields, bracket, fraction):
    var_count, level_count, row_count, lons = fields.shape
    plev_count = bracket.shape[0]
    own = row_count // lon_count
    width = var_count * plev_count
    dma = pltpu.SemaphoreType.DMA
    anywhere = pl.BlockSpec(memory_space=pl.ANY)
    room = 2 * fields.size + 4 * bracket.size + 2 * fraction.size * (1 + var_count)
    in_vmem = pl.BlockSpec(memory_space=pltpu.VMEM)
    rows_shape = (var_count, own, plev_count, lons * lon_count)
    mean_shape = (var_count, own, plev_count)
    inputs = [pltpu.with_memory_space_constraint(x, pltpu.HBM) for x in (fields, bracket, fraction)]
    held = pl.pallas_call(
        functools.partial(exchange, lon_count, lat_count, float(lons * lon_count)),
        out_shape=(
            pltpu.VMEM(rows_shape, jnp.bfloat16),
            pltpu.VMEM(mean_shape, jnp.float32),
            pltpu.VMEM(mean_shape, jnp.float32),
        ),
        in_specs=[anywhere] * 3,
        out_specs=(in_vmem,) * 3,
        scratch_shapes=[
            pltpu.VMEM((var_count // 2, level_count, 2 * row_count, lons), fields.dtype),
            pltpu.VMEM(bracket.shape, bracket.dtype),
            pltpu.VMEM(fraction.shape, fraction.dtype),
            pltpu.VMEM((var_count, row_count, plev_count, lons), jnp.bfloat16),
            pltpu.VMEM((row_count + 2, 1, width), jnp.float32),
            pltpu.VMEM((lon_count, own + 2, 1, width), jnp.float32),
            pltpu.VMEM((lon_count, 1, width), jnp.float32),
            dma((1,)),
            dma((var_count // 2,)),
            dma((1,)),
            dma((1,)),
            dma((1,)),
            dma((1,)),
            pltpu.SemaphoreType.REGULAR,
        ],
        compiler_params=pltpu.CompilerParams(
            collective_id=0, has_side_effects=True, vmem_limit_bytes=room + (8 << 20)
        ),
    )(*inputs)
    held = [pltpu.with_memory_space_constraint(x, pltpu.VMEM) for x in held]
    on_pressure, zonal_mean, meridional = pl.pallas_call(
        finish,
        out_shape=(
            jax.ShapeDtypeStruct(rows_shape, jnp.bfloat16),
            jax.ShapeDtypeStruct(mean_shape, jnp.float32),
            jax.ShapeDtypeStruct(mean_shape, jnp.float32),
        ),
        in_specs=[in_vmem] * 3,
        out_specs=(anywhere,) * 3,
        scratch_shapes=[dma((1,))],
        compiler_params=pltpu.CompilerParams(vmem_limit_bytes=8 << 20),
    )(*held)
    return (
        on_pressure.transpose(0, 2, 1, 3),
        zonal_mean.transpose(0, 2, 1),
        meridional.transpose(0, 2, 1),
    )


def solution(mesh):
    return jax.shard_map(
        functools.partial(shards, mesh.shape["lon"], mesh.shape["lat"]),
        mesh=mesh,
        in_specs=(P(None, None, "lat", "lon"), P(None, "lat", "lon"), P(None, "lat", "lon")),
        out_specs=(
            P(None, None, ("lat", "lon"), None),
            P(None, None, ("lat", "lon")),
            P(None, None, ("lat", "lon")),
        ),
        check_vma=False,
    )
```
